128 devices in a mesh: head: 4 (over z_hi, core), seq: 32 (over y, x, z_lo).
Axes of the slice: x: 4, y: 4, z: 4 (z_hi: 2, z_lo: 2; z = z_hi * 2 + z_lo), core: 2. Of those that a mesh axis runs over, the one named last changes fastest.
Arguments:
- skip_stream: bfloat16 [4096, 4096], P('head', 'seq'), may hold values from -6 to 6
- acceptance_vector: bfloat16 [4096, 4096], P('head', 'seq'), may hold values from -6 to 6
- address_vectors: bfloat16 [4096, 4096], P('head', 'seq'), may hold values from -0.75 to 0.75
- content_vectors: bfloat16 [4096, 4096], P('head', 'seq'), may hold values from -6 to 6
- emission_valve: bfloat16 [4096, 4096], P('head', 'seq'), may hold values from -6 to 6
- fading_exponent: bfloat16 [4096, 4096], P('head', 'seq'), may hold values from -0.7 to 0
- adaptation_speed: bfloat16 [4096, 4096], P('head', 'seq'), may hold values from 0 to 0.9
- erasure_factor: float32 [4096], P('head'), may hold values from 0.3 to 3
- reward_coefficient: float32 [4096], P('head'), may hold values from -4 to 4
- cluster_multiplier: float32 [4096], P('head'), may hold values from 0.5 to 2
- cluster_offset: float32 [4096], P('head'), may hold values from -3 to 3
- projection_weights: bfloat16 [4096, 4096], P(None, 'head'), may hold values from -0.125 to 0.125
Outputs:
- layer_output: bfloat16 [4096, 4096], P('head', 'seq')
The draws below stay inside these ranges and needn't reach their ends.
All inputs are finite; a program needn't handle non-finite values.
Results may differ from the reference program's by a relative error of at most 0.0048.
Values may be sent and summed in bfloat16 or wider, within the bound.
A program may use at most 128 MiB of HBM per device.

```python
import math
import jax
import jax.numpy as jnp
from jax import lax

EMBED_DIMENSION = 4096
ATTENTION_UNITS = 64
UNIT_CHANNELS = 64
TOK_DEV = 128
TOKEN_COUNT = 4096


def head_classes(key):
    order = jax.random.permutation(jax.random.fold_in(key, 101), ATTENTION_UNITS)
    fast_count = ATTENTION_UNITS // 2
    return order >= fast_count


def unit_ranks(key):
    unit_keys = jax.random.split(jax.random.fold_in(key, 107), ATTENTION_UNITS)
    return jax.vmap(lambda unit_key: jax.random.permutation(unit_key, UNIT_CHANNELS))(unit_keys)


def long_channels(key):
    return unit_ranks(key) >= UNIT_CHANNELS - UNIT_CHANNELS // 4


def quick_channels(key):
    ranks = unit_ranks(key)
    return jnp.logical_and(ranks >= UNIT_CHANNELS // 4, ranks < UNIT_CHANNELS // 2)


def steady_places(key):
    chosen = unit_ranks(key) < UNIT_CHANNELS // 4
    slab_count = TOKEN_COUNT // TOK_DEV
    slab_pick = jax.random.randint(jax.random.fold_in(key, 108), (ATTENTION_UNITS, UNIT_CHANNELS, slab_count), 0, 4) == 0
    slab_pick = jnp.repeat(slab_pick, TOK_DEV, axis=2)
    return jnp.logical_and(chosen[:, :, None], slab_pick)


def draw_fading_exponent(key, part):
    slow_heads = head_classes(key)
    keeps_long = jnp.logical_or(slow_heads[:, None], long_channels(key))
    factor = jnp.exp(jax.random.uniform(jax.random.fold_in(key, 102), (ATTENTION_UNITS, UNIT_CHANNELS, TOKEN_COUNT), jnp.float32, -math.log(2.0), math.log(2.0)))
    sequential_field = -0.4 / TOKEN_COUNT * factor
    fast_field = -2.3 / 40.0 * factor
    places = jax.random.randint(jax.random.fold_in(key, 103), (2,), 0, TOKEN_COUNT)
    removed_state = jnp.any(jnp.arange(TOKEN_COUNT)[:, None] == places[None, :], axis=1)
    block_outputs = jnp.log(jax.random.uniform(jax.random.fold_in(key, 104), (ATTENTION_UNITS, UNIT_CHANNELS, TOKEN_COUNT), jnp.float32, 0.5, 0.8))
    sequential_field = jnp.where(removed_state[None, None, :], block_outputs, sequential_field)
    field = jnp.where(keeps_long[:, :, None], sequential_field, fast_field)
    steady_field = jax.random.uniform(jax.random.fold_in(key, 109), (ATTENTION_UNITS, UNIT_CHANNELS, TOKEN_COUNT), jnp.float32, -0.7, -0.69)
    field = jnp.where(steady_places(key), steady_field, field)
    return field.reshape(EMBED_DIMENSION, TOKEN_COUNT).astype(jnp.bfloat16)


def draw_adaptation_speed(key, part):
    slow_heads = head_classes(key)
    slow_rate = jnp.where(slow_heads[:, None], jnp.logical_not(quick_channels(key)), long_channels(key))
    factor = jnp.exp(jax.random.uniform(jax.random.fold_in(key, 105), (ATTENTION_UNITS, UNIT_CHANNELS, TOKEN_COUNT), jnp.float32, -math.log(2.0), math.log(2.0)))
    sequential_field = 32.0 / TOKEN_COUNT * factor
    fast_field = jnp.exp(jax.random.uniform(jax.random.fold_in(key, 106), (ATTENTION_UNITS, UNIT_CHANNELS, TOKEN_COUNT), jnp.float32, math.log(0.05), math.log(0.9)))
    quick_field = jnp.exp(jax.random.uniform(jax.random.fold_in(key, 110), (ATTENTION_UNITS, UNIT_CHANNELS, TOKEN_COUNT), jnp.float32, math.log(0.2), math.log(0.9)))
    rapid_field = jnp.where(slow_heads[:, None, None], quick_field, fast_field)
    field = jnp.where(slow_rate[:, :, None], sequential_field, rapid_field)
    return field.reshape(EMBED_DIMENSION, TOKEN_COUNT).astype(jnp.bfloat16)


def strengthened(entries, key, source, target, parts, factor):
    owner, partner = [(jnp.arange(entries.shape[dim]) // (entries.shape[dim] // parts)).reshape([-1 if axis == dim else 1 for axis in range(entries.ndim)]) for dim in (source, target)]
    chosen = jax.random.permutation(key, parts)[partner]
    strong = (owner == chosen) | (owner == (partner + parts // 2) % parts)
    return jnp.where(strong, factor * entries, entries)


def shard_levels(stream_key, shape, shards, low, top_value):
    def one(position, parts):
        steps = jax.random.uniform(jax.random.fold_in(jax.random.fold_in(stream_key, 6), position), (parts,), jnp.float32, low / len(shards), top_value / len(shards))
        return jnp.repeat(jnp.exp(steps), shape[position] // parts).reshape((-1,) + (1,) * (len(shape) - position - 1))

    gain = one(*shards[0])
    for cut in shards[1:]:
        gain = gain * one(*cut)
    return gain


def bell_draw(key, dims, scale, most, cuts=(), kind=jnp.bfloat16):
    values = scale * jax.random.normal(key, dims, jnp.float32)
    if cuts:
        values = values * shard_levels(key, dims, cuts, -0.22, 0.18)
    return jnp.clip(values, -most, most).astype(kind)


def heavy_noise(stream_key, dims, width, bound, pieces, heavy, kind=jnp.bfloat16):
    values = width * jax.random.normal(stream_key, dims, jnp.float32)
    if pieces:
        values = values * shard_levels(stream_key, dims, pieces, -0.22, 0.18)
    return jnp.clip(strengthened(values, jax.random.fold_in(stream_key, 3), *heavy), -bound, bound).astype(kind)


def setup_inputs(seed: int = 0) -> dict:
    key_of = jax.random.split(jax.random.key(seed), 13)
    skip_stream = bell_draw(key_of[0], (EMBED_DIMENSION, TOKEN_COUNT), 1.0, 6.0, ((0, 4), (1, 32)))
    acceptance_vector = bell_draw(key_of[1], (EMBED_DIMENSION, TOKEN_COUNT), 1.0, 6.0, ((0, 4), (1, 32)))
    address_vectors = bell_draw(key_of[2], (EMBED_DIMENSION, TOKEN_COUNT), 0.125, 0.75, ((0, 4), (1, 32)))
    content_vectors = bell_draw(key_of[3], (EMBED_DIMENSION, TOKEN_COUNT), 1.0, 6.0, ((0, 4), (1, 32)))
    emission_valve = bell_draw(key_of[4], (EMBED_DIMENSION, TOKEN_COUNT), 1.0, 6.0, ((0, 4), (1, 32)))
    fading_exponent = draw_fading_exponent(jax.random.fold_in(key_of[12], 71), 0)
    adaptation_speed = draw_adaptation_speed(jax.random.fold_in(key_of[12], 71), 0)
    erasure_factor = jnp.clip(jnp.exp(math.log(3.0) - 2.3025851 * jax.random.uniform(key_of[7], (EMBED_DIMENSION,), jnp.float32) ** shard_levels(key_of[7], (EMBED_DIMENSION,), ((0, 4),), -0.2, 0.2)), 0.3, 3.0)
    reward_coefficient = bell_draw(key_of[8], (EMBED_DIMENSION,), 1.0, 4.0, ((0, 4),), jnp.float32)
    cluster_multiplier = jnp.clip(jnp.exp(math.log(2.0) - 1.3862944 * jax.random.uniform(key_of[9], (EMBED_DIMENSION,), jnp.float32) ** shard_levels(key_of[9], (EMBED_DIMENSION,), ((0, 4),), -0.2, 0.2)), 0.5, 2.0)
    cluster_offset = bell_draw(key_of[10], (EMBED_DIMENSION,), 0.5, 3.0, ((0, 4),), jnp.float32)
    projection_weights = heavy_noise(key_of[11], (EMBED_DIMENSION, EMBED_DIMENSION), EMBED_DIMENSION ** -0.5, 0.125, ((1, 4),), (1, 0, 4, 2.0))
    return {"skip_stream": skip_stream, "acceptance_vector": acceptance_vector, "address_vectors": address_vectors, "content_vectors": content_vectors, "emission_valve": emission_valve, "fading_exponent": fading_exponent, "adaptation_speed": adaptation_speed, "erasure_factor": erasure_factor, "reward_coefficient": reward_coefficient, "cluster_multiplier": cluster_multiplier, "cluster_offset": cluster_offset, "projection_weights": projection_weights}


HIGHEST = lax.Precision.HIGHEST

def position_results(field):
    return jnp.transpose(field.astype(jnp.float32).reshape(ATTENTION_UNITS, UNIT_CHANNELS, TOK_DEV), (2, 0, 1))

def as_blocks(field):
    return jnp.transpose(field.reshape(field.shape[0], TOKEN_COUNT // TOK_DEV, TOK_DEV), (1, 0, 2))

def wkv_step(memory, token_item):
    recept_now, key_now, value_now, decay_now, removal_now, rate_now = token_item
    removed = jnp.einsum('hvk,hk->hv', memory, removal_now, precision=HIGHEST)
    memory = memory * jnp.exp(decay_now)[:, None, :] - removed[:, :, None] * (removal_now * rate_now)[:, None, :] + value_now[:, :, None] * key_now[:, None, :]
    return (memory, jnp.einsum('hvk,hk->hv', memory, recept_now, precision=HIGHEST))

def reference(skip_stream, acceptance_vector, address_vectors, content_vectors, emission_valve, fading_exponent, adaptation_speed, erasure_factor, reward_coefficient, cluster_multiplier, cluster_offset, projection_weights):
    scale_heads = erasure_factor.reshape(ATTENTION_UNITS, UNIT_CHANNELS)
    reward_each_unit = reward_coefficient.reshape(ATTENTION_UNITS, UNIT_CHANNELS)
    gain_heads = cluster_multiplier.reshape(ATTENTION_UNITS, UNIT_CHANNELS)
    bias_heads = cluster_offset.reshape(ATTENTION_UNITS, UNIT_CHANNELS)

    def run_block(memory, block_item):
        recept_part, key_part, value_part, valve_portion, decay_part, rate_part = block_item
        acceptance_column = position_results(recept_part)
        address_column = position_results(key_part)
        content_column = position_results(value_part)
        decay_tok = position_results(decay_part)
        rate_tok = position_results(rate_part)
        scaled = address_column * scale_heads
        removal = scaled * lax.rsqrt(lax.optimization_barrier(jnp.sum(scaled * scaled, axis=2, keepdims=True)) + 1e-06)
        memory, read_out = lax.scan(wkv_step, memory, (acceptance_column, address_column, content_column, decay_tok, removal, rate_tok))
        centre = lax.optimization_barrier(jnp.mean(read_out, axis=2, keepdims=True))
        centred = read_out - centre
        spread = lax.optimization_barrier(jnp.mean(centred * centred, axis=2, keepdims=True))
        standardised = centred * lax.rsqrt(spread + 0.00064) * gain_heads + bias_heads
        reward_addend = lax.optimization_barrier(jnp.sum(acceptance_column * address_column * reward_each_unit, axis=2, keepdims=True)) * content_column
        blended_content = (standardised + reward_addend) * position_results(valve_portion)
        blended_content = jnp.transpose(blended_content, (1, 2, 0)).reshape(EMBED_DIMENSION, TOK_DEV).astype(jnp.bfloat16)
        return (memory, blended_content)
    start = jnp.zeros((ATTENTION_UNITS, UNIT_CHANNELS, UNIT_CHANNELS), jnp.float32)
    final_memory, mixed_blocks = lax.scan(run_block, start, (as_blocks(acceptance_vector), as_blocks(address_vectors), as_blocks(content_vectors), as_blocks(emission_valve), as_blocks(fading_exponent), as_blocks(adaptation_speed)))
    blended_content = jnp.transpose(mixed_blocks, (1, 0, 2)).reshape(EMBED_DIMENSION, TOKEN_COUNT)
    projected = jnp.dot(projection_weights, blended_content, preferred_element_type=jnp.float32)
    return (projected + skip_stream.astype(jnp.float32)).astype(jnp.bfloat16)
```

```python
import functools
import jax
import jax.numpy as jnp
from jax import lax
from jax.experimental import pallas as pl
from jax.experimental.pallas import tpu as pltpu
from jax.sharding import PartitionSpec as P

MESH = pl.DeviceIdType.MESH
CH = 64
HEADS = 16
TOK = 128
SLABS = 32
ROWS = 1024
GROUP = 8
CHUNK = 256
F32 = jnp.float32
BF16 = jnp.bfloat16


def dot(left, right, dims=((1,), (0,)), precision=lax.Precision.HIGH):
    return lax.dot_general(
        left, right, (dims, ((), ())), precision=precision, preferred_element_type=F32
    )


def kernel(
    skip_ref, r_ref, k_ref, v_ref, g_ref, w_ref, a_ref, ef_ref, rc_ref, gm_ref, gb_ref, wt_hbm,
    out_ref,
    par, comb, read, local, inbox, prefix, outbox, entering, mixed, weights,
    send_a, got_a, held_b, send_b, got_b, total,
    wt_sem, comb_send, comb_recv, state_send, state_recv, rs_send, rs_recv,
):
    head = lax.axis_index("head")
    me = lax.axis_index("seq")
    core = lax.rem(head, 2)
    pair = head // 2

    def owner_of(h):
        y, x = h // 4, lax.rem(h, 4)
        return y * 8 + x * 2 + lax.rem(x + y + core, 2)

    barrier = pltpu.get_barrier_semaphore()

    def greet(d, carry):
        pl.semaphore_signal(
            barrier, inc=1, device_id=(head, lax.rem(me + d, SLABS)), device_id_type=MESH
        )
        return carry

    lax.fori_loop(1, SLABS, greet, 0)

    def greet_head(d, carry):
        pl.semaphore_signal(
            barrier, inc=1, device_id=(lax.rem(head + d, 4), me), device_id_type=MESH
        )
        return carry

    lax.fori_loop(1, 4, greet_head, 0)
    wt_copy = pltpu.make_async_copy(wt_hbm, weights, wt_sem)
    wt_copy.start()

    for p, ref in enumerate((ef_ref, rc_ref, gm_ref, gb_ref)):
        for j in range(8):
            par[p, j * 128 : (j + 1) * 128, :] = jnp.broadcast_to(ref[j : j + 1, :], (128, 128)).T

    row = lax.broadcasted_iota(jnp.int32, (TOK, TOK), 0)
    col = lax.broadcasted_iota(jnp.int32, (TOK, TOK), 1)
    upto = jnp.where(row <= col, 1.0, 0.0).astype(BF16)
    eye = (
        lax.broadcasted_iota(jnp.int32, (CH, CH), 0) == lax.broadcasted_iota(jnp.int32, (CH, CH), 1)
    )

    def head_local(h):
        rows = pl.ds(pl.multiple_of(h * CH, CH), CH)
        w16 = w_ref[rows, :]
        running = dot(w16, upto, precision=None)
        wf = w16.astype(F32)
        kf = k_ref[rows, :].astype(F32)
        vf = v_ref[rows, :].astype(F32)
        rf = r_ref[rows, :].astype(F32)
        scaled = kf * par[0, rows, :]
        removal = scaled * lax.rsqrt(jnp.sum(scaled * scaled, axis=0, keepdims=True) + 1e-6)
        pulled = removal * a_ref[rows, :].astype(F32)
        mid = running[:, 63:64]
        end = running[:, 127:128]
        back = jnp.exp(mid - running)
        fwd = jnp.exp(running - mid)
        fwd_before = jnp.exp(running - wf - mid)
        at_mid = jnp.exp(mid)
        to_end = back * jnp.exp(end - mid)
        removal_fwd = -removal * fwd_before
        recept_fwd = rf * fwd
        ahead = jnp.concatenate([removal_fwd, recept_fwd], axis=1)
        from_pull = dot(pulled * back, ahead, ((0,), (0,)))
        from_key = dot(kf * back, ahead, ((0,), (0,)))
        pair_mix = jnp.where(row < col, from_pull[:, :TOK], 0.0)
        pair_read = jnp.where(row <= col, from_pull[:, TOK:], 0.0)
        key_mix = jnp.where(row < col, from_key[:, :TOK], 0.0)
        key_read = jnp.where(row <= col, from_key[:, TOK:], 0.0)
        apart = row ^ col
        inverse = jnp.where(apart == 1, pair_mix, 0.0)
        for level in range(1, 7):
            off = jnp.where((apart >> level) == 1, pair_mix, 0.0)
            joined = off + dot(inverse, off)
            inverse = inverse + joined + dot(joined, inverse)
        seen = jnp.concatenate([dot(vf, key_mix), removal_fwd * at_mid], axis=0)
        solved = seen + dot(seen, inverse)
        written = jnp.concatenate(
            [
                solved,
                jnp.concatenate([vf, jnp.zeros((CH, TOK), F32)], axis=0),
            ],
            axis=1,
        )
        ends = jnp.concatenate([pulled * to_end, kf * to_end], axis=1)
        ops = dot(written, ends, ((1,), (1,)))
        state = ops[:CH]
        trans = ops[CH:] + jnp.where(eye, jnp.exp(end), 0.0)
        comb[h] = jnp.concatenate([trans, state], axis=1)
        reads = dot(written, jnp.concatenate([pair_read, key_read], axis=0))
        local[h] = reads[:CH]
        read[h] = reads[CH:] + recept_fwd * at_mid

    def comb_copy(h):
        return pltpu.make_async_remote_copy(
            src_ref=comb.at[h],
            dst_ref=inbox.at[me],
            send_sem=comb_send.at[h],
            recv_sem=comb_recv.at[me],
            device_id=(head, owner_of(h)),
            device_id_type=MESH,
        )

    def send_comb(h):
        @pl.when(owner_of(h) != me)
        def _():
            comb_copy(h).start()

        @pl.when(owner_of(h) == me)
        def _():
            inbox[me] = comb[h]

    head_local(0)
    pl.semaphore_wait(barrier, SLABS - 1 + 3)

    def one_head(h, carry):
        head_local(h)
        send_comb(h - 1)
        return carry

    lax.fori_loop(1, HEADS, one_head, 0)
    send_comb(HEADS - 1)

    my_head = (me // 8) * 4 + lax.rem(me // 2, 4)

    def state_copy(i):
        return pltpu.make_async_remote_copy(
            src_ref=outbox.at[i],
            dst_ref=entering.at[my_head],
            send_sem=state_send.at[i],
            recv_sem=state_recv.at[my_head],
            device_id=(head, i),
            device_id_type=MESH,
        )

    @pl.when(owner_of(my_head) == me)
    def _():
        def arrive(d, carry):
            i = lax.rem(me + d, SLABS)
            pltpu.make_async_remote_copy(
                src_ref=comb.at[0],
                dst_ref=inbox.at[i],
                send_sem=comb_send.at[0],
                recv_sem=comb_recv.at[i],
                device_id=(head, i),
                device_id_type=MESH,
            ).wait_recv()
            return carry

        lax.fori_loop(1, SLABS, arrive, 0)

        def pack(i, value):
            outbox[i] = jnp.concatenate([value[: CH // 2], value[CH // 2 :]], axis=1)

        groups = SLABS // GROUP
        for g in range(groups):
            item = inbox[g * GROUP]
            prefix[g * GROUP] = jnp.concatenate([item[:, CH:], item[:, :CH]], axis=0)

        def step(i, carry):
            for g in range(groups):
                item = inbox[g * GROUP + i]
                moved = dot(prefix[g * GROUP + i - 1], item[:, :CH])
                prefix[g * GROUP + i] = moved + jnp.concatenate(
                    [item[:, CH:], jnp.zeros((CH, CH), F32)], axis=0
                )
            return carry

        lax.fori_loop(1, GROUP, step, 0)
        start = jnp.zeros((CH, CH), F32)
        starts = [start]
        for g in range(groups - 1):
            done = prefix[g * GROUP + GROUP - 1]
            start = dot(start, done[CH:]) + done[:CH]
            starts.append(start)
        for g in range(groups):
            pack(g * GROUP, starts[g])
            for i in range(1, GROUP):
                done = prefix[g * GROUP + i - 1]
                pack(g * GROUP + i, dot(starts[g], done[CH:]) + done[:CH])

        def give(d, carry):
            state_copy(lax.rem(me + d, SLABS)).start()
            return carry

        lax.fori_loop(1, SLABS, give, 0)
        entering[my_head] = outbox[me]

    def finish_head(h, carry):
        rows = pl.ds(pl.multiple_of(h * CH, CH), CH)

        @pl.when(owner_of(h) != me)
        def _():
            pltpu.make_async_remote_copy(
                src_ref=outbox.at[0],
                dst_ref=entering.at[h],
                send_sem=state_send.at[0],
                recv_sem=state_recv.at[h],
                device_id=(head, owner_of(h)),
                device_id_type=MESH,
            ).wait_recv()

        packed = entering[h]
        state = jnp.concatenate([packed[:, :CH], packed[:, CH:]], axis=0)
        y = local[h] + dot(state, read[h])
        centred = y - jnp.mean(y, axis=0, keepdims=True)
        spread = jnp.mean(centred * centred, axis=0, keepdims=True)
        normed = centred * lax.rsqrt(spread + 0.00064) * par[2, rows, :] + par[3, rows, :]
        kf = k_ref[rows, :].astype(F32)
        vf = v_ref[rows, :].astype(F32)
        rf = r_ref[rows, :].astype(F32)
        bonus = jnp.sum(rf * kf * par[1, rows, :], axis=0, keepdims=True) * vf
        mixed[rows, :] = ((normed + bonus) * g_ref[rows, :].astype(F32)).astype(BF16)
        return carry

    lax.fori_loop(0, HEADS, finish_head, 0)

    wt_copy.wait()
    partner = pair * 2 + 1 - core
    across = (1 - pair) * 2 + core

    def piece(dest, c):
        rows = pl.ds(pl.multiple_of(dest * ROWS + c * CHUNK, CHUNK), CHUNK)
        return dot(weights[rows, :], mixed[...], precision=None)

    pieces = ROWS // CHUNK

    def near_copy(c):
        return pltpu.make_async_remote_copy(
            src_ref=send_a.at[c],
            dst_ref=got_a.at[c],
            send_sem=rs_send.at[c],
            recv_sem=rs_recv.at[c],
            device_id=(partner, me),
            device_id_type=MESH,
        )

    def far_copy(c):
        return pltpu.make_async_remote_copy(
            src_ref=send_b.at[c],
            dst_ref=got_b.at[c],
            send_sem=rs_send.at[2 * pieces + c],
            recv_sem=rs_recv.at[2 * pieces + c],
            device_id=(across, me),
            device_id_type=MESH,
        )

    for c in range(pieces):
        send_a[c] = piece((1 - pair) * 2 + 1 - core, c)
        near_copy(c).start()
    for c in range(pieces):
        held_b[c] = piece(across, c)
        near_copy(c).wait_recv()
        send_b[c] = (held_b[c] + got_a[c]).astype(BF16)
        far_copy(c).start()
    for c in range(pieces):
        send_a[pieces + c] = piece(partner, c)
        near_copy(pieces + c).start()
    for c in range(pieces):
        rows = slice(c * CHUNK, (c + 1) * CHUNK)
        total[rows, :] = piece(head, c) + skip_ref[rows, :].astype(F32)
        near_copy(pieces + c).wait_recv()
        total[rows, :] = total[rows, :] + got_a[pieces + c]
    for c in range(pieces):
        rows = slice(c * CHUNK, (c + 1) * CHUNK)
        far_copy(c).wait_recv()
        out_ref[rows, :] = (total[rows, :] + got_b[c].astype(F32)).astype(BF16)

    for c in range(2 * pieces):
        near_copy(c).wait_send()
    for c in range(pieces):
        far_copy(c).wait_send()

    def sent_comb(h, carry):
        @pl.when(owner_of(h) != me)
        def _():
            comb_copy(h).wait_send()

        return carry

    lax.fori_loop(0, HEADS, sent_comb, 0)

    @pl.when(owner_of(my_head) == me)
    def _():
        def sent_state(d, carry):
            state_copy(lax.rem(me + d, SLABS)).wait_send()
            return carry

        lax.fori_loop(1, SLABS, sent_state, 0)


def on_device(skip, r, k, v, g, w, a, ef, rc, gm, gb, wt):
    vmem = pl.BlockSpec(memory_space=pltpu.VMEM)
    pieces = ROWS // CHUNK
    dma = pltpu.SemaphoreType.DMA
    return pl.pallas_call(
        kernel,
        out_shape=jax.ShapeDtypeStruct((ROWS, TOK), BF16),
        in_specs=[vmem] * 11 + [pl.BlockSpec(memory_space=pl.ANY)],
        out_specs=vmem,
        scratch_shapes=[
            pltpu.VMEM((4, ROWS, TOK), F32),
            pltpu.VMEM((HEADS, CH, 2 * CH), F32),
            pltpu.VMEM((HEADS, CH, TOK), F32),
            pltpu.VMEM((HEADS, CH, TOK), F32),
            pltpu.VMEM((SLABS, CH, 2 * CH), F32),
            pltpu.VMEM((SLABS, 2 * CH, CH), F32),
            pltpu.VMEM((SLABS, CH // 2, 2 * CH), F32),
            pltpu.VMEM((HEADS, CH // 2, 2 * CH), F32),
            pltpu.VMEM((ROWS, TOK), BF16),
            pltpu.VMEM((4 * ROWS, ROWS), BF16),
            pltpu.VMEM((2 * pieces, CHUNK, TOK), F32),
            pltpu.VMEM((2 * pieces, CHUNK, TOK), F32),
            pltpu.VMEM((pieces, CHUNK, TOK), F32),
            pltpu.VMEM((pieces, CHUNK, TOK), BF16),
            pltpu.VMEM((pieces, CHUNK, TOK), BF16),
            pltpu.VMEM((ROWS, TOK), F32),
            dma(()),
            dma((HEADS,)),
            dma((SLABS,)),
            dma((SLABS,)),
            dma((HEADS,)),
            dma((3 * pieces,)),
            dma((3 * pieces,)),
        ],
        compiler_params=pltpu.CompilerParams(
            collective_id=0, has_side_effects=True, vmem_limit_bytes=60000 * 1024
        ),
    )(skip, r, k, v, g, w, a, *(p.reshape(8, 128) for p in (ef, rc, gm, gb)), wt)


def solution(mesh):
    split = P("head", "seq")
    vec = P("head")
    return jax.shard_map(
        on_device,
        mesh=mesh,
        in_specs=(split,) * 7 + (vec,) * 4 + (P(None, "head"),),
        out_specs=split,
        check_vma=False,
    )
```

```python
import functools
import jax
import jax.numpy as jnp
from jax import lax
from jax.experimental import pallas as pl
from jax.experimental.pallas import tpu as pltpu
from jax.sharding import PartitionSpec as P

MESH = pl.DeviceIdType.MESH
CH = 64
HEADS = 16
TOK = 128
SLABS = 32
ROWS = 1024
GROUP = 8
BATCH = 8
CHUNK = 256
F32 = jnp.float32
BF16 = jnp.bfloat16


def dot(left, right, dims=((1,), (0,)), precision=lax.Precision.HIGH):
    return lax.dot_general(
        left, right, (dims, ((), ())), precision=precision, preferred_element_type=F32
    )


def halves(x):
    high = x.astype(BF16)
    return high, (x - high.astype(F32)).astype(BF16)


def fold(x):
    return x[:, :TOK] + x[:, TOK:]


def mm(left, right):
    return jnp.dot(left, right, preferred_element_type=F32)


def kernel(
    skip_ref, r_ref, k_ref, v_ref, g_ref, w_ref, a_ref, ef_ref, rc_ref, gm_ref, gb_ref, wt_hbm,
    out_ref,
    par, comb, read, local, inbox, prefix, outbox, entering, mixed, weights,
    send_a, got_a, held_b, send_b, got_b, total,
    masks, pull_t, key_t, ends_t, ahead_s, pair_s, pread_s, kread_s, inv_s, inv, part_s, seen_s,
    recv_s,
    wt_sem, comb_send, comb_recv, state_send, state_recv, rs_send, rs_recv,
):
    head = lax.axis_index("head")
    me = lax.axis_index("seq")
    core = lax.rem(head, 2)
    pair = head // 2

    def owner_of(h):
        y, x = h // 4, lax.rem(h, 4)
        return y * 8 + x * 2 + lax.rem(x + y + core, 2)

    barrier = pltpu.get_barrier_semaphore()

    def greet(d, carry):
        pl.semaphore_signal(
            barrier, inc=1, device_id=(head, lax.rem(me + d, SLABS)), device_id_type=MESH
        )
        return carry

    lax.fori_loop(1, SLABS, greet, 0)

    def greet_head(d, carry):
        pl.semaphore_signal(
            barrier, inc=1, device_id=(lax.rem(head + d, 4), me), device_id_type=MESH
        )
        return carry

    lax.fori_loop(1, 4, greet_head, 0)
    wt_copy = pltpu.make_async_copy(wt_hbm, weights, wt_sem)
    wt_copy.start()

    for p, ref in enumerate((ef_ref, rc_ref, gm_ref, gb_ref)):
        for j in range(8):
            par[p, j * 128 : (j + 1) * 128, :] = jnp.broadcast_to(ref[j : j + 1, :], (128, 128)).T

    row = lax.broadcasted_iota(jnp.int32, (TOK, TOK), 0)
    col = lax.broadcasted_iota(jnp.int32, (TOK, TOK), 1)
    upto = jnp.where(row <= col, 1.0, 0.0).astype(BF16)
    for level in range(7):
        masks[level] = jnp.where(((row ^ col) >> level) == 1, 1.0, 0.0).astype(BF16)
    zero = jnp.zeros((TOK, TOK), BF16)
    diag = lax.broadcasted_iota(jnp.int32, (CH, TOK), 0) == lax.broadcasted_iota(
        jnp.int32, (CH, TOK), 1
    )
    left_half = lax.broadcasted_iota(jnp.int32, (CH, TOK), 1) < CH

    def wide(pair):
        return jnp.concatenate(
            [
                jnp.concatenate([pair[:, :TOK], pair[:, TOK:]], axis=1),
                jnp.concatenate([pair[:, :TOK], zero], axis=1),
            ],
            axis=0,
        )

    def beside(x):
        return jnp.concatenate(halves(x), axis=1)

    def turned(x):
        return jnp.concatenate(halves(x), axis=0).T

    def group_local(base):
        for i in range(BATCH):
            rows = slice((base + i) * CH, (base + i + 1) * CH)
            w16 = w_ref[rows, :]
            running = mm(w16, upto)
            kf = k_ref[rows, :].astype(F32)
            scaled = kf * par[0, rows, :]
            removal = scaled * lax.rsqrt(jnp.sum(scaled * scaled, axis=0, keepdims=True) + 1e-6)
            pulled = removal * a_ref[rows, :].astype(F32)
            mid = running[:, 63:64]
            end = running[:, 127:128]
            back = jnp.exp(mid - running)
            at_mid = jnp.exp(mid)
            to_end = back * jnp.exp(end - mid)
            removal_fwd = -removal * jnp.exp(running - w16.astype(F32) - mid)
            recept_fwd = r_ref[rows, :].astype(F32) * jnp.exp(running - mid)
            pull_t[i] = turned(pulled * back)
            key_t[i] = turned(kf * back)
            ends_t[i, :, :TOK] = turned(pulled * to_end)
            ends_t[i, :, TOK:] = turned(kf * to_end)
            rem_hi, rem_lo = halves(removal_fwd)
            rec_hi, rec_lo = halves(recept_fwd)
            ahead_s[i, :CH, :TOK] = rem_hi
            ahead_s[i, CH:, :TOK] = rem_lo
            ahead_s[i, :CH, TOK:] = rec_hi
            ahead_s[i, CH:, TOK:] = rec_lo
            seen_s[i, CH:, :] = removal_fwd * at_mid
            recv_s[i] = recept_fwd * at_mid
            comb[base + i] = jnp.where(diag, jnp.exp(end), 0.0)
        for i in range(BATCH):
            ahead = ahead_s[i]
            ahead = jnp.concatenate([ahead[:CH], ahead[:CH], ahead[CH:], ahead[CH:]], axis=0)
            pull = pull_t[i]
            from_pull = mm(jnp.concatenate([pull, pull], axis=1), ahead)
            pair_mix = jnp.where(row < col, from_pull[:, :TOK], 0.0)
            pair_s[i] = beside(pair_mix)
            start = jnp.where(row == col, 1.0, pair_mix * masks[0].astype(F32))
            inv[i] = start
            inv_s[i] = beside(start)
            pread_s[i] = beside(jnp.where(row <= col, from_pull[:, TOK:], 0.0))
            key = key_t[i]
            from_key = mm(jnp.concatenate([key, key], axis=1), ahead)
            kread_s[i] = beside(jnp.where(row <= col, from_key[:, TOK:], 0.0))
            part_s[i] = beside(jnp.where(row < col, from_key[:, :TOK], 0.0))
        for i in range(BATCH):
            rows = slice((base + i) * CH, (base + i + 1) * CH)
            seen_s[i, :CH, :] = fold(mm(v_ref[rows, :], part_s[i]))
        for level in range(1, 7):
            mask = masks[level]
            for i in range(BATCH):
                off = pair_s[i] * jnp.concatenate([mask, mask], axis=1)
                part_s[i] = beside(fold(mm(inv_s[i], wide(off))))
            for i in range(BATCH):
                new = inv[i] + fold(mm(part_s[i], wide(inv_s[i])))
                if level < 6:
                    inv[i] = new
                inv_s[i] = beside(new)
        for i in range(BATCH):
            part_s[i] = beside(fold(mm(beside(seen_s[i]), wide(inv_s[i]))))
        for i in range(BATCH):
            h = base + i
            rows = slice(h * CH, (h + 1) * CH)
            pread = pread_s[i]
            pull_end = ends_t[i, :, :TOK]
            solved = part_s[i]
            out = mm(
                solved,
                jnp.concatenate(
                    [
                        jnp.concatenate([pull_end, pread], axis=1),
                        jnp.concatenate([pull_end, pread[:, :TOK], zero], axis=1),
                    ],
                    axis=0,
                ),
            )
            kread = kread_s[i]
            v16 = v_ref[rows, :]
            direct = mm(
                jnp.concatenate([v16, v16], axis=1),
                jnp.concatenate(
                    [
                        jnp.concatenate([ends_t[i, :, TOK:], kread[:, :TOK]], axis=1),
                        jnp.concatenate([zero, kread[:, TOK:]], axis=1),
                    ],
                    axis=0,
                ),
            )
            state = out[:CH, :TOK] + direct[:, :TOK]
            trans = out[CH:, :TOK]
            state = state + pltpu.roll(state, CH, 1)
            trans = trans + pltpu.roll(trans, CH, 1)
            comb[h] = jnp.where(left_half, trans + comb[h], state)
            local[h] = fold(out[:CH, TOK:]) + direct[:, TOK:]
            read[h] = jnp.concatenate(halves(fold(out[CH:, TOK:]) + recv_s[i]), axis=0)

    def comb_copy(h):
        return pltpu.make_async_remote_copy(
            src_ref=comb.at[h],
            dst_ref=inbox.at[me],
            send_sem=comb_send.at[h],
            recv_sem=comb_recv.at[me],
            device_id=(head, owner_of(h)),
            device_id_type=MESH,
        )

    def send_comb(h, carry):
        @pl.when(owner_of(h) != me)
        def _():
            comb_copy(h).start()

        @pl.when(owner_of(h) == me)
        def _():
            inbox[me] = comb[h]

        return carry

    for base in range(0, HEADS, BATCH):
        group_local(base)
        if base == 0:
            pl.semaphore_wait(barrier, SLABS - 1 + 3)
        lax.fori_loop(base, base + BATCH, send_comb, 0)

    my_head = (me // 8) * 4 + lax.rem(me // 2, 4)

    def state_copy(i):
        return pltpu.make_async_remote_copy(
            src_ref=outbox.at[i],
            dst_ref=entering.at[my_head],
            send_sem=state_send.at[i],
            recv_sem=state_recv.at[my_head],
            device_id=(head, i),
            device_id_type=MESH,
        )

    @pl.when(owner_of(my_head) == me)
    def _():
        def arrive(d, carry):
            i = lax.rem(me + d, SLABS)
            pltpu.make_async_remote_copy(
                src_ref=comb.at[0],
                dst_ref=inbox.at[i],
                send_sem=comb_send.at[0],
                recv_sem=comb_recv.at[i],
                device_id=(head, i),
                device_id_type=MESH,
            ).wait_recv()
            return carry

        lax.fori_loop(1, SLABS, arrive, 0)

        def pack(i, value):
            outbox[i] = beside(value)

        groups = SLABS // GROUP
        for g in range(groups):
            item = inbox[g * GROUP]
            prefix[g * GROUP] = jnp.concatenate([item[:, CH:], item[:, :CH]], axis=0)

        def step(i, carry):
            for g in range(groups):
                item = inbox[g * GROUP + i]
                moved = dot(prefix[g * GROUP + i - 1], item[:, :CH])
                prefix[g * GROUP + i] = moved + jnp.concatenate(
                    [item[:, CH:], jnp.zeros((CH, CH), F32)], axis=0
                )
            return carry

        lax.fori_loop(1, GROUP, step, 0)
        start = jnp.zeros((CH, CH), F32)
        starts = [start]
        for g in range(groups - 1):
            done = prefix[g * GROUP + GROUP - 1]
            start = dot(start, done[CH:]) + done[:CH]
            starts.append(start)
        for g in range(groups):
            pack(g * GROUP, starts[g])
            for i in range(1, GROUP):
                done = prefix[g * GROUP + i - 1]
                pack(g * GROUP + i, dot(starts[g], done[CH:]) + done[:CH])

        def give(d, carry):
            state_copy(lax.rem(me + d, SLABS)).start()
            return carry

        lax.fori_loop(1, SLABS, give, 0)
        entering[my_head] = outbox[me]

    def arrived(h):
        @pl.when(owner_of(h) != me)
        def _():
            pltpu.make_async_remote_copy(
                src_ref=outbox.at[0],
                dst_ref=entering.at[h],
                send_sem=state_send.at[0],
                recv_sem=state_recv.at[h],
                device_id=(head, owner_of(h)),
                device_id_type=MESH,
            ).wait_recv()

    for base in range(0, HEADS, BATCH):
        for i in range(BATCH):
            arrived(base + i)
        outs = []
        for i in range(BATCH):
            reading = read[base + i]
            state = entering[base + i]
            y = mm(
                jnp.concatenate([state, state], axis=1),
                jnp.concatenate([reading[:CH], reading[:CH], reading[CH:], reading[CH:]], axis=0),
            )
            outs.append(y + local[base + i])
        for i in range(BATCH):
            rows = slice((base + i) * CH, (base + i + 1) * CH)
            y = outs[i]
            centred = y - jnp.mean(y, axis=0, keepdims=True)
            spread = jnp.mean(centred * centred, axis=0, keepdims=True)
            normed = centred * lax.rsqrt(spread + 0.00064) * par[2, rows, :] + par[3, rows, :]
            kf = k_ref[rows, :].astype(F32)
            vf = v_ref[rows, :].astype(F32)
            rf = r_ref[rows, :].astype(F32)
            bonus = jnp.sum(rf * kf * par[1, rows, :], axis=0, keepdims=True) * vf
            mixed[rows, :] = ((normed + bonus) * g_ref[rows, :].astype(F32)).astype(BF16)

    wt_copy.wait()
    partner = pair * 2 + 1 - core
    across = (1 - pair) * 2 + core

    def piece(dest, c):
        rows = pl.ds(pl.multiple_of(dest * ROWS + c * CHUNK, CHUNK), CHUNK)
        return dot(weights[rows, :], mixed[...], precision=None)

    pieces = ROWS // CHUNK

    def near_copy(c):
        return pltpu.make_async_remote_copy(
            src_ref=send_a.at[c],
            dst_ref=got_a.at[c],
            send_sem=rs_send.at[c],
            recv_sem=rs_recv.at[c],
            device_id=(partner, me),
            device_id_type=MESH,
        )

    def far_copy(c):
        return pltpu.make_async_remote_copy(
            src_ref=send_b.at[c],
            dst_ref=got_b.at[c],
            send_sem=rs_send.at[2 * pieces + c],
            recv_sem=rs_recv.at[2 * pieces + c],
            device_id=(across, me),
            device_id_type=MESH,
        )

    for c in range(pieces):
        send_a[c] = piece((1 - pair) * 2 + 1 - core, c)
        near_copy(c).start()
    for c in range(pieces):
        held_b[c] = piece(across, c)
        near_copy(c).wait_recv()
        send_b[c] = (held_b[c] + got_a[c]).astype(BF16)
        far_copy(c).start()
    for c in range(pieces):
        send_a[pieces + c] = piece(partner, c)
        near_copy(pieces + c).start()
    for c in range(pieces):
        rows = slice(c * CHUNK, (c + 1) * CHUNK)
        total[rows, :] = piece(head, c) + skip_ref[rows, :].astype(F32)
        near_copy(pieces + c).wait_recv()
        total[rows, :] = total[rows, :] + got_a[pieces + c]
    for c in range(pieces):
        rows = slice(c * CHUNK, (c + 1) * CHUNK)
        far_copy(c).wait_recv()
        out_ref[rows, :] = (total[rows, :] + got_b[c].astype(F32)).astype(BF16)

    for c in range(2 * pieces):
        near_copy(c).wait_send()
    for c in range(pieces):
        far_copy(c).wait_send()

    def sent_comb(h, carry):
        @pl.when(owner_of(h) != me)
        def _():
            comb_copy(h).wait_send()

        return carry

    lax.fori_loop(0, HEADS, sent_comb, 0)

    @pl.when(owner_of(my_head) == me)
    def _():
        def sent_state(d, carry):
            state_copy(lax.rem(me + d, SLABS)).wait_send()
            return carry

        lax.fori_loop(1, SLABS, sent_state, 0)


def on_device(skip, r, k, v, g, w, a, ef, rc, gm, gb, wt):
    vmem = pl.BlockSpec(memory_space=pltpu.VMEM)
    pieces = ROWS // CHUNK
    dma = pltpu.SemaphoreType.DMA
    return pl.pallas_call(
        kernel,
        out_shape=jax.ShapeDtypeStruct((ROWS, TOK), BF16),
        in_specs=[vmem] * 11 + [pl.BlockSpec(memory_space=pl.ANY)],
        out_specs=vmem,
        scratch_shapes=[
            pltpu.VMEM((4, ROWS, TOK), F32),
            pltpu.VMEM((HEADS, CH, 2 * CH), F32),
            pltpu.VMEM((HEADS, 2 * CH, TOK), BF16),
            pltpu.VMEM((HEADS, CH, TOK), F32),
            pltpu.VMEM((SLABS, CH, 2 * CH), F32),
            pltpu.VMEM((SLABS, 2 * CH, CH), F32),
            pltpu.VMEM((SLABS, CH, 2 * CH), BF16),
            pltpu.VMEM((HEADS, CH, 2 * CH), BF16),
            pltpu.VMEM((ROWS, TOK), BF16),
            pltpu.VMEM((4 * ROWS, ROWS), BF16),
            pltpu.VMEM((2 * pieces, CHUNK, TOK), F32),
            pltpu.VMEM((2 * pieces, CHUNK, TOK), F32),
            pltpu.VMEM((pieces, CHUNK, TOK), F32),
            pltpu.VMEM((pieces, CHUNK, TOK), BF16),
            pltpu.VMEM((pieces, CHUNK, TOK), BF16),
            pltpu.VMEM((ROWS, TOK), F32),
            pltpu.VMEM((7, TOK, TOK), BF16),
            pltpu.VMEM((BATCH, TOK, TOK), BF16),
            pltpu.VMEM((BATCH, TOK, TOK), BF16),
            pltpu.VMEM((BATCH, TOK, 2 * TOK), BF16),
            pltpu.VMEM((BATCH, TOK, 2 * TOK), BF16),
            pltpu.VMEM((BATCH, TOK, 2 * TOK), BF16),
            pltpu.VMEM((BATCH, TOK, 2 * TOK), BF16),
            pltpu.VMEM((BATCH, TOK, 2 * TOK), BF16),
            pltpu.VMEM((BATCH, TOK, 2 * TOK), BF16),
            pltpu.VMEM((BATCH, TOK, TOK), F32),
            pltpu.VMEM((BATCH, TOK, 2 * TOK), BF16),
            pltpu.VMEM((BATCH, TOK, TOK), F32),
            pltpu.VMEM((BATCH, CH, TOK), F32),
            dma(()),
            dma((HEADS,)),
            dma((SLABS,)),
            dma((SLABS,)),
            dma((HEADS,)),
            dma((3 * pieces,)),
            dma((3 * pieces,)),
        ],
        compiler_params=pltpu.CompilerParams(
            collective_id=0, has_side_effects=True, vmem_limit_bytes=60000 * 1024
        ),
    )(skip, r, k, v, g, w, a, *(p.reshape(8, 128) for p in (ef, rc, gm, gb)), wt)


def solution(mesh):
    split = P("head", "seq")
    vec = P("head")
    return jax.shard_map(
        on_device,
        mesh=mesh,
        in_specs=(split,) * 7 + (vec,) * 4 + (P(None, "head"),),
        out_specs=split,
        check_vma=False,
    )
```

```python
import functools
import jax
import jax.numpy as jnp
from jax import lax
from jax.experimental import pallas as pl
from jax.experimental.pallas import tpu as pltpu
from jax.sharding import PartitionSpec as P

MESH = pl.DeviceIdType.MESH
CH = 64
HEADS = 16
TOK = 128
SLABS = 32
ROWS = 1024
EXTRA = 16
GROUP = 8
BATCH = 8
CHUNK = 256
F32 = jnp.float32
BF16 = jnp.bfloat16


def dot(left, right, dims=((1,), (0,)), precision=lax.Precision.HIGH):
    return lax.dot_general(
        left, right, (dims, ((), ())), precision=precision, preferred_element_type=F32
    )


def halves(x):
    high = x.astype(BF16)
    return high, (x - high.astype(F32)).astype(BF16)


def fold(x):
    return x[:, :TOK] + x[:, TOK:]


def mm(left, right):
    return jnp.dot(left, right, preferred_element_type=F32)


def kernel(
    skip_ref, r_ref, k_ref, v_ref, g_ref, w_ref, a_ref, ef_ref, rc_ref, gm_ref, gb_ref, wt_hbm,
    out_ref,
    par, comb, read, local, inbox, prefix, outbox, entering, mixed, weights,
    send_a, got_a, held_b, send_b, got_b, total,
    masks, pull_t, key_t, ends_t, ahead_s, pair_s, pread_s, kread_s, inv_s, inv, part_s, seen_s,
    recv_s, decay_s, solved_s, rest,
    wt_sem, comb_send, comb_recv, state_send, state_recv, rs_send, rs_recv,
):
    head = lax.axis_index("head")
    me = lax.axis_index("seq")
    core = lax.rem(head, 2)
    pair = head // 2

    def owner_of(h):
        odd, place = h // 8, h % 8
        y = place // 2
        x = 2 * (place % 2) + (y + odd) % 2
        return y * 8 + x * 2 + (odd + core) % 2

    barrier = pltpu.get_barrier_semaphore()

    def greet(d, carry):
        pl.semaphore_signal(
            barrier, inc=1, device_id=(head, lax.rem(me + d, SLABS)), device_id_type=MESH
        )
        return carry

    lax.fori_loop(1, SLABS, greet, 0)

    def greet_head(d, carry):
        pl.semaphore_signal(
            barrier, inc=1, device_id=(lax.rem(head + d, 4), me), device_id_type=MESH
        )
        return carry

    lax.fori_loop(1, 4, greet_head, 0)
    wt_copy = pltpu.make_async_copy(wt_hbm, weights, wt_sem)
    wt_copy.start()

    def spread(p, ref):
        for j in range(8):
            par[p, j * 128 : (j + 1) * 128, :] = jnp.broadcast_to(ref[j : j + 1, :], (128, 128)).T

    spread(0, ef_ref)

    row = lax.broadcasted_iota(jnp.int32, (TOK, TOK), 0)
    col = lax.broadcasted_iota(jnp.int32, (TOK, TOK), 1)
    upto = jnp.where(row <= col, 1.0, 0.0).astype(BF16)
    for level in range(7):
        masks[level] = jnp.where(((row ^ col) >> level) == 1, 1.0, 0.0).astype(BF16)
    zero = jnp.zeros((TOK, TOK), BF16)
    diag = lax.broadcasted_iota(jnp.int32, (CH, TOK), 0) == lax.broadcasted_iota(
        jnp.int32, (CH, TOK), 1
    )
    left_half = lax.broadcasted_iota(jnp.int32, (CH, TOK), 1) < CH

    def wide(pair):
        return jnp.concatenate(
            [
                jnp.concatenate([pair[:, :TOK], pair[:, TOK:]], axis=1),
                jnp.concatenate([pair[:, :TOK], zero], axis=1),
            ],
            axis=0,
        )

    def beside(x):
        return jnp.concatenate(halves(x), axis=1)

    def turned(x):
        return jnp.concatenate(halves(x), axis=0).T

    def group_local(base):
        for i in range(BATCH):
            rows = slice((base + i) * CH, (base + i + 1) * CH)
            w16 = w_ref[rows, :]
            running = mm(w16, upto)
            kf = k_ref[rows, :].astype(F32)
            scaled = kf * par[0, rows, :]
            removal = scaled * lax.rsqrt(jnp.sum(scaled * scaled, axis=0, keepdims=True) + 1e-6)
            pulled = removal * a_ref[rows, :].astype(F32)
            mid = running[:, 63:64]
            end = running[:, 127:128]
            back = jnp.exp(mid - running)
            at_mid = jnp.exp(mid)
            to_end = back * jnp.exp(end - mid)
            removal_fwd = -removal * jnp.exp(running - w16.astype(F32) - mid)
            recept_fwd = r_ref[rows, :].astype(F32) * jnp.exp(running - mid)
            pull_t[i] = turned(pulled * back)
            key_t[i] = turned(kf * back)
            ends_t[i, :, :TOK] = turned(pulled * to_end)
            ends_t[i, :, TOK:] = turned(kf * to_end)
            rem_hi, rem_lo = halves(removal_fwd)
            rec_hi, rec_lo = halves(recept_fwd)
            ahead_s[i, :CH, :TOK] = rem_hi
            ahead_s[i, CH:, :TOK] = rem_lo
            ahead_s[i, :CH, TOK:] = rec_hi
            ahead_s[i, CH:, TOK:] = rec_lo
            seen_s[i, CH:, :] = removal_fwd * at_mid
            recv_s[base + i] = recept_fwd * at_mid
            decay_s[i] = jnp.where(diag, jnp.exp(end), 0.0)
        for i in range(BATCH):
            ahead = ahead_s[i]
            ahead = jnp.concatenate([ahead[:CH], ahead[:CH], ahead[CH:], ahead[CH:]], axis=0)
            pull = pull_t[i]
            from_pull = mm(jnp.concatenate([pull, pull], axis=1), ahead)
            pair_mix = jnp.where(row < col, from_pull[:, :TOK], 0.0)
            pair_s[i] = beside(pair_mix)
            start = jnp.where(row == col, 1.0, pair_mix * masks[0].astype(F32))
            inv[i] = start
            inv_s[i] = beside(start)
            pread_s[base + i] = from_pull[:, TOK:]
            key = key_t[i]
            from_key = mm(jnp.concatenate([key, key], axis=1), ahead)
            kread_s[base + i] = from_key[:, TOK:]
            part_s[i] = beside(jnp.where(row < col, from_key[:, :TOK], 0.0))
        for i in range(BATCH):
            rows = slice((base + i) * CH, (base + i + 1) * CH)
            seen_s[i, :CH, :] = fold(mm(v_ref[rows, :], part_s[i]))
        for level in range(1, 7):
            mask = masks[level]
            for i in range(BATCH):
                off = pair_s[i] * jnp.concatenate([mask, mask], axis=1)
                part_s[i] = beside(fold(mm(inv_s[i], wide(off))))
            for i in range(BATCH):
                new = inv[i] + fold(mm(part_s[i], wide(inv_s[i])))
                if level < 6:
                    inv[i] = new
                inv_s[i] = beside(new)
        for i in range(BATCH):
            solved_s[base + i] = beside(fold(mm(beside(seen_s[i]), wide(inv_s[i]))))
        for i in range(BATCH):
            h = base + i
            rows = slice(h * CH, (h + 1) * CH)
            pull_end = ends_t[i, :, :TOK]
            ops = mm(solved_s[h], jnp.concatenate([pull_end, pull_end], axis=0))
            state = ops[:CH] + mm(v_ref[rows, :], ends_t[i, :, TOK:])
            trans = ops[CH:]
            state = state + pltpu.roll(state, CH, 1)
            trans = trans + pltpu.roll(trans, CH, 1) + decay_s[i]
            sent = jnp.where(left_half, trans, state).astype(BF16)
            comb[h, :CH, :] = sent
            missed = jnp.where(diag, trans - sent.astype(F32), 0.0)
            comb[h, CH:, :] = jnp.broadcast_to(
                jnp.sum(missed, axis=0, keepdims=True), (EXTRA, TOK)
            ).astype(BF16)

    def group_read(base):
        for i in range(BATCH):
            h = base + i
            rows = slice(h * CH, (h + 1) * CH)
            pread = beside(jnp.where(row <= col, pread_s[h], 0.0))
            kread = beside(jnp.where(row <= col, kread_s[h], 0.0))
            out = fold(mm(solved_s[h], wide(pread)))
            local[h] = out[:CH] + fold(mm(v_ref[rows, :], kread))
            read[h] = jnp.concatenate(halves(out[CH:] + recv_s[h]), axis=0)
            kf = k_ref[rows, :].astype(F32)
            vf = v_ref[rows, :].astype(F32)
            rf = r_ref[rows, :].astype(F32)
            bonus = jnp.sum(rf * kf * par[1, rows, :], axis=0, keepdims=True) * vf
            rest[h] = bonus + par[3, rows, :]

    def comb_copy(h):
        return pltpu.make_async_remote_copy(
            src_ref=comb.at[h],
            dst_ref=inbox.at[me],
            send_sem=comb_send.at[h],
            recv_sem=comb_recv.at[me],
            device_id=(head, owner_of(h)),
            device_id_type=MESH,
        )

    def send_comb(t, carry):
        h = (t // BATCH) * BATCH + (t + me + 3 * (me // 8)) % BATCH

        @pl.when(owner_of(h) != me)
        def _():
            comb_copy(h).start()

        @pl.when(owner_of(h) == me)
        def _():
            inbox[me] = comb[h]

        return carry

    for base in range(0, HEADS, BATCH):
        group_local(base)
        if base == 0:
            pl.semaphore_wait(barrier, SLABS - 1 + 3)
        lax.fori_loop(base, base + BATCH, send_comb, 0)
    spread(1, rc_ref)
    spread(2, gm_ref)
    spread(3, gb_ref)
    for base in range(0, HEADS, BATCH):
        group_read(base)

    my_y, my_x = me // 8, (me // 2) % 4
    my_head = ((my_x + my_y) % 2) * 8 + 2 * my_y + my_x // 2

    def state_copy(i):
        return pltpu.make_async_remote_copy(
            src_ref=outbox.at[i],
            dst_ref=entering.at[my_head],
            send_sem=state_send.at[i],
            recv_sem=state_recv.at[my_head],
            device_id=(head, i),
            device_id_type=MESH,
        )

    @pl.when(owner_of(my_head) == me)
    def _():
        def arrive(d, carry):
            i = lax.rem(me + d, SLABS)
            pltpu.make_async_remote_copy(
                src_ref=comb.at[0],
                dst_ref=inbox.at[i],
                send_sem=comb_send.at[0],
                recv_sem=comb_recv.at[i],
                device_id=(head, i),
                device_id_type=MESH,
            ).wait_recv()
            return carry

        lax.fori_loop(1, SLABS, arrive, 0)

        def pack(i, value):
            value = value.astype(BF16)
            outbox[i] = jnp.concatenate([value[: CH // 2], value[CH // 2 :]], axis=1)

        def item_of(i):
            item = inbox[i]
            trans = item[:CH, :CH]
            state = pltpu.roll(item[:CH].astype(F32), CH, 1)[:, :CH]
            return trans, item[CH : CH + 1, :CH].astype(F32), state

        groups = SLABS // GROUP
        for g in range(groups):
            trans, missed, state = item_of(g * GROUP)
            whole = trans.astype(F32) + jnp.where(diag[:, :CH], missed, 0.0)
            prefix[g * GROUP] = jnp.concatenate([state, whole], axis=0)

        def step(i, carry):
            for g in range(groups):
                trans, missed, state = item_of(g * GROUP + i)
                old = prefix[g * GROUP + i - 1]
                high, low = halves(old)
                moved = mm(high, trans) + mm(low, trans) + old * missed
                prefix[g * GROUP + i, :CH, :] = moved[:CH] + state
                prefix[g * GROUP + i, CH:, :] = moved[CH:]
            return carry

        lax.fori_loop(1, GROUP, step, 0)
        start = jnp.zeros((CH, CH), F32)
        starts = [start]
        for g in range(groups - 1):
            done = prefix[g * GROUP + GROUP - 1]
            start = dot(start, done[CH:]) + done[:CH]
            starts.append(start)
        for g in range(groups):
            pack(g * GROUP, starts[g])
            for i in range(1, GROUP):
                done = prefix[g * GROUP + i - 1]
                pack(g * GROUP + i, dot(starts[g], done[CH:]) + done[:CH])

        def give(d, carry):
            state_copy(lax.rem(me + d, SLABS)).start()
            return carry

        lax.fori_loop(1, SLABS, give, 0)
        entering[my_head] = outbox[me]

    def arrived(h):
        @pl.when(owner_of(h) != me)
        def _():
            pltpu.make_async_remote_copy(
                src_ref=outbox.at[0],
                dst_ref=entering.at[h],
                send_sem=state_send.at[0],
                recv_sem=state_recv.at[h],
                device_id=(head, owner_of(h)),
                device_id_type=MESH,
            ).wait_recv()

    for base in range(0, HEADS, BATCH):
        for i in range(BATCH):
            arrived(base + i)
        outs = []
        for i in range(BATCH):
            reading = read[base + i]
            state = entering[base + i]
            nil = jnp.zeros((CH, TOK), BF16)
            upper = jnp.concatenate([reading[:CH], nil, reading[CH:], nil], axis=0)
            lower = jnp.concatenate([nil, reading[:CH], nil, reading[CH:]], axis=0)
            y = mm(
                jnp.concatenate([state, state], axis=1),
                jnp.concatenate([upper, lower], axis=1),
            )
            outs.append(jnp.concatenate([y[:, :TOK], y[:, TOK:]], axis=0) + local[base + i])
        for i in range(BATCH):
            rows = slice((base + i) * CH, (base + i + 1) * CH)
            y = outs[i]
            centred = y - jnp.mean(y, axis=0, keepdims=True)
            spreading = jnp.mean(centred * centred, axis=0, keepdims=True)
            normed = centred * lax.rsqrt(spreading + 0.00064) * par[2, rows, :]
            mixed[rows, :] = ((normed + rest[base + i]) * g_ref[rows, :].astype(F32)).astype(BF16)

    wt_copy.wait()
    partner = pair * 2 + 1 - core
    across = (1 - pair) * 2 + core

    def piece(dest, c):
        rows = pl.ds(pl.multiple_of(dest * ROWS + c * CHUNK, CHUNK), CHUNK)
        return dot(weights[rows, :], mixed[...], precision=None)

    pieces = ROWS // CHUNK

    def near_copy(c):
        return pltpu.make_async_remote_copy(
            src_ref=send_a.at[c],
            dst_ref=got_a.at[c],
            send_sem=rs_send.at[c],
            recv_sem=rs_recv.at[c],
            device_id=(partner, me),
            device_id_type=MESH,
        )

    def far_copy(c):
        return pltpu.make_async_remote_copy(
            src_ref=send_b.at[c],
            dst_ref=got_b.at[c],
            send_sem=rs_send.at[2 * pieces + c],
            recv_sem=rs_recv.at[2 * pieces + c],
            device_id=(across, me),
            device_id_type=MESH,
        )

    for c in range(pieces):
        send_a[c] = piece((1 - pair) * 2 + 1 - core, c)
        near_copy(c).start()
    for c in range(pieces):
        held_b[c] = piece(across, c)
        near_copy(c).wait_recv()
        send_b[c] = (held_b[c] + got_a[c]).astype(BF16)
        far_copy(c).start()
    for c in range(pieces):
        send_a[pieces + c] = piece(partner, c)
        near_copy(pieces + c).start()
    for c in range(pieces):
        rows = slice(c * CHUNK, (c + 1) * CHUNK)
        total[rows, :] = piece(head, c) + skip_ref[rows, :].astype(F32)
        near_copy(pieces + c).wait_recv()
        total[rows, :] = total[rows, :] + got_a[pieces + c]
    for c in range(pieces):
        rows = slice(c * CHUNK, (c + 1) * CHUNK)
        far_copy(c).wait_recv()
        out_ref[rows, :] = (total[rows, :] + got_b[c].astype(F32)).astype(BF16)

    for c in range(2 * pieces):
        near_copy(c).wait_send()
    for c in range(pieces):
        far_copy(c).wait_send()

    def sent_comb(h, carry):
        @pl.when(owner_of(h) != me)
        def _():
            comb_copy(h).wait_send()

        return carry

    lax.fori_loop(0, HEADS, sent_comb, 0)

    @pl.when(owner_of(my_head) == me)
    def _():
        def sent_state(d, carry):
            state_copy(lax.rem(me + d, SLABS)).wait_send()
            return carry

        lax.fori_loop(1, SLABS, sent_state, 0)


def on_device(skip, r, k, v, g, w, a, ef, rc, gm, gb, wt):
    vmem = pl.BlockSpec(memory_space=pltpu.VMEM)
    pieces = ROWS // CHUNK
    dma = pltpu.SemaphoreType.DMA
    return pl.pallas_call(
        kernel,
        out_shape=jax.ShapeDtypeStruct((ROWS, TOK), BF16),
        in_specs=[vmem] * 11 + [pl.BlockSpec(memory_space=pl.ANY)],
        out_specs=vmem,
        scratch_shapes=[
            pltpu.VMEM((4, ROWS, TOK), F32),
            pltpu.VMEM((HEADS, CH + EXTRA, 2 * CH), BF16),
            pltpu.VMEM((HEADS, 2 * CH, TOK), BF16),
            pltpu.VMEM((HEADS, CH, TOK), F32),
            pltpu.VMEM((SLABS, CH + EXTRA, 2 * CH), BF16),
            pltpu.VMEM((SLABS, 2 * CH, CH), F32),
            pltpu.VMEM((SLABS, CH // 2, 2 * CH), BF16),
            pltpu.VMEM((HEADS, CH // 2, 2 * CH), BF16),
            pltpu.VMEM((ROWS, TOK), BF16),
            pltpu.VMEM((4 * ROWS, ROWS), BF16),
            pltpu.VMEM((2 * pieces, CHUNK, TOK), F32),
            pltpu.VMEM((2 * pieces, CHUNK, TOK), F32),
            pltpu.VMEM((pieces, CHUNK, TOK), F32),
            pltpu.VMEM((pieces, CHUNK, TOK), BF16),
            pltpu.VMEM((pieces, CHUNK, TOK), BF16),
            pltpu.VMEM((ROWS, TOK), F32),
            pltpu.VMEM((7, TOK, TOK), BF16),
            pltpu.VMEM((BATCH, TOK, TOK), BF16),
            pltpu.VMEM((BATCH, TOK, TOK), BF16),
            pltpu.VMEM((BATCH, TOK, 2 * TOK), BF16),
            pltpu.VMEM((BATCH, TOK, 2 * TOK), BF16),
            pltpu.VMEM((BATCH, TOK, 2 * TOK), BF16),
            pltpu.VMEM((HEADS, TOK, TOK), F32),
            pltpu.VMEM((HEADS, TOK, TOK), F32),
            pltpu.VMEM((BATCH, TOK, 2 * TOK), BF16),
            pltpu.VMEM((BATCH, TOK, TOK), F32),
            pltpu.VMEM((BATCH, TOK, 2 * TOK), BF16),
            pltpu.VMEM((BATCH, TOK, TOK), F32),
            pltpu.VMEM((HEADS, CH, TOK), F32),
            pltpu.VMEM((BATCH, CH, TOK), F32),
            pltpu.VMEM((HEADS, TOK, 2 * TOK), BF16),
            pltpu.VMEM((HEADS, CH, TOK), F32),
            dma(()),
            dma((HEADS,)),
            dma((SLABS,)),
            dma((SLABS,)),
            dma((HEADS,)),
            dma((3 * pieces,)),
            dma((3 * pieces,)),
        ],
        compiler_params=pltpu.CompilerParams(
            collective_id=0, has_side_effects=True, vmem_limit_bytes=40 * 1024 * 1024
        ),
    )(skip, r, k, v, g, w, a, *(p.reshape(8, 128) for p in (ef, rc, gm, gb)), wt)


def solution(mesh):
    split = P("head", "seq")
    vec = P("head")
    return jax.shard_map(
        on_device,
        mesh=mesh,
        in_specs=(split,) * 7 + (vec,) * 4 + (P(None, "head"),),
        out_specs=split,
        check_vma=False,
    )
```

```python
import functools
import jax
import jax.numpy as jnp
from jax import lax
from jax.experimental import pallas as pl
from jax.experimental.pallas import tpu as pltpu
from jax.sharding import PartitionSpec as P

MESH = pl.DeviceIdType.MESH
CH = 64
HEADS = 16
TOK = 128
SLABS = 32
ROWS = 1024
EXTRA = 16
GROUP = 8
BATCH = 8
CHUNK = 256
F32 = jnp.float32
BF16 = jnp.bfloat16


def dot(left, right, dims=((1,), (0,)), precision=lax.Precision.HIGH):
    return lax.dot_general(
        left, right, (dims, ((), ())), precision=precision, preferred_element_type=F32
    )


def halves(x):
    high = x.astype(BF16)
    return high, (x - high.astype(F32)).astype(BF16)


def fold(x):
    return x[:, :TOK] + x[:, TOK:]


def mm(left, right):
    return jnp.dot(left, right, preferred_element_type=F32)


def kernel(
    skip_hbm, r_hbm, k_hbm, v_hbm, g_hbm, w_hbm, a_hbm, ef_hbm, rc_hbm, gm_hbm, gb_hbm, wt_hbm,
    out_ref,
    skip_ref, r_ref, k_ref, v_ref, g_ref, w_ref, a_ref, ef_ref, rc_ref, gm_ref, gb_ref,
    par, comb, read, local, inbox, prefix, outbox, entering, mixed, weights,
    send_a, got_a, held_b, send_b, got_b, total,
    masks, pull_t, key_t, ends_t, ahead_s, pair_s, pread_s, kread_s, inv_s, inv, part_s, seen_s,
    recv_s, decay_s, solved_s, rest,
    in_sem, wt_sem, comb_send, comb_recv, state_send, state_recv, rs_send, rs_recv,
):
    head = lax.axis_index("head")
    me = lax.axis_index("seq")
    core = lax.rem(head, 2)
    pair = head // 2

    def owner_of(h):
        odd, place = h // 8, h % 8
        y = place // 2
        x = 2 * (place % 2) + (y + odd) % 2
        return y * 8 + x * 2 + (odd + core) % 2

    first = ((ef_hbm, ef_ref), (w_hbm, w_ref), (k_hbm, k_ref), (a_hbm, a_ref), (r_hbm, r_ref), (v_hbm, v_ref))
    second = ((rc_hbm, rc_ref), (gm_hbm, gm_ref), (gb_hbm, gb_ref), (g_hbm, g_ref), (skip_hbm, skip_ref))
    first = [pltpu.make_async_copy(*pair, in_sem.at[n]) for n, pair in enumerate(first)]
    second = [pltpu.make_async_copy(*pair, in_sem.at[6 + n]) for n, pair in enumerate(second)]
    wt_copy = pltpu.make_async_copy(wt_hbm, weights, wt_sem)
    for copy in first + second + [wt_copy]:
        copy.start()

    barrier = pltpu.get_barrier_semaphore()

    def greet(d, carry):
        pl.semaphore_signal(
            barrier, inc=1, device_id=(head, lax.rem(me + d, SLABS)), device_id_type=MESH
        )
        return carry

    lax.fori_loop(1, SLABS, greet, 0)

    def greet_head(d, carry):
        pl.semaphore_signal(
            barrier, inc=1, device_id=(lax.rem(head + d, 4), me), device_id_type=MESH
        )
        return carry

    lax.fori_loop(1, 4, greet_head, 0)

    def spread(p, ref):
        for j in range(8):
            par[p, j * 128 : (j + 1) * 128, :] = jnp.broadcast_to(ref[j : j + 1, :], (128, 128)).T

    for copy in first:
        copy.wait()
    spread(0, ef_ref)

    row = lax.broadcasted_iota(jnp.int32, (TOK, TOK), 0)
    col = lax.broadcasted_iota(jnp.int32, (TOK, TOK), 1)
    upto = jnp.where(row <= col, 1.0, 0.0).astype(BF16)
    for level in range(7):
        masks[level] = jnp.where(((row ^ col) >> level) == 1, 1.0, 0.0).astype(BF16)
    zero = jnp.zeros((TOK, TOK), BF16)
    diag = lax.broadcasted_iota(jnp.int32, (CH, TOK), 0) == lax.broadcasted_iota(
        jnp.int32, (CH, TOK), 1
    )
    left_half = lax.broadcasted_iota(jnp.int32, (CH, TOK), 1) < CH

    def wide(pair):
        return jnp.concatenate(
            [
                jnp.concatenate([pair[:, :TOK], pair[:, TOK:]], axis=1),
                jnp.concatenate([pair[:, :TOK], zero], axis=1),
            ],
            axis=0,
        )

    def beside(x):
        return jnp.concatenate(halves(x), axis=1)

    def turned(x):
        return jnp.concatenate(halves(x), axis=0).T

    def group_local(base):
        for i in range(BATCH):
            rows = slice((base + i) * CH, (base + i + 1) * CH)
            w16 = w_ref[rows, :]
            running = mm(w16, upto)
            kf = k_ref[rows, :].astype(F32)
            scaled = kf * par[0, rows, :]
            removal = scaled * lax.rsqrt(jnp.sum(scaled * scaled, axis=0, keepdims=True) + 1e-6)
            pulled = removal * a_ref[rows, :].astype(F32)
            mid = running[:, 63:64]
            end = running[:, 127:128]
            back = jnp.exp(mid - running)
            at_mid = jnp.exp(mid)
            to_end = back * jnp.exp(end - mid)
            removal_fwd = -removal * jnp.exp(running - w16.astype(F32) - mid)
            recept_fwd = r_ref[rows, :].astype(F32) * jnp.exp(running - mid)
            pull_t[i] = turned(pulled * back)
            key_t[i] = turned(kf * back)
            ends_t[i, :, :TOK] = turned(pulled * to_end)
            ends_t[i, :, TOK:] = turned(kf * to_end)
            rem_hi, rem_lo = halves(removal_fwd)
            rec_hi, rec_lo = halves(recept_fwd)
            ahead_s[i, :CH, :TOK] = rem_hi
            ahead_s[i, CH:, :TOK] = rem_lo
            ahead_s[i, :CH, TOK:] = rec_hi
            ahead_s[i, CH:, TOK:] = rec_lo
            seen_s[i, CH:, :] = removal_fwd * at_mid
            recv_s[base + i] = recept_fwd * at_mid
            decay_s[i] = jnp.where(diag, jnp.exp(end), 0.0)
        for i in range(BATCH):
            ahead = ahead_s[i]
            ahead = jnp.concatenate([ahead[:CH], ahead[:CH], ahead[CH:], ahead[CH:]], axis=0)
            pull = pull_t[i]
            from_pull = mm(jnp.concatenate([pull, pull], axis=1), ahead)
            pair_mix = jnp.where(row < col, from_pull[:, :TOK], 0.0)
            pair_s[i] = beside(pair_mix)
            start = jnp.where(row == col, 1.0, pair_mix * masks[0].astype(F32))
            inv[i] = start
            inv_s[i] = beside(start)
            pread_s[base + i] = from_pull[:, TOK:]
            key = key_t[i]
            from_key = mm(jnp.concatenate([key, key], axis=1), ahead)
            kread_s[base + i] = from_key[:, TOK:]
            part_s[i] = beside(jnp.where(row < col, from_key[:, :TOK], 0.0))
        for i in range(BATCH):
            rows = slice((base + i) * CH, (base + i + 1) * CH)
            seen_s[i, :CH, :] = fold(mm(v_ref[rows, :], part_s[i]))
        for level in range(1, 7):
            mask = masks[level]
            for i in range(BATCH):
                off = pair_s[i] * jnp.concatenate([mask, mask], axis=1)
                part_s[i] = beside(fold(mm(inv_s[i], wide(off))))
            for i in range(BATCH):
                new = inv[i] + fold(mm(part_s[i], wide(inv_s[i])))
                if level < 6:
                    inv[i] = new
                inv_s[i] = beside(new)
        for i in range(BATCH):
            solved_s[base + i] = beside(fold(mm(beside(seen_s[i]), wide(inv_s[i]))))
        for i in range(BATCH):
            h = base + i
            rows = slice(h * CH, (h + 1) * CH)
            pull_end = ends_t[i, :, :TOK]
            ops = mm(solved_s[h], jnp.concatenate([pull_end, pull_end], axis=0))
            state = ops[:CH] + mm(v_ref[rows, :], ends_t[i, :, TOK:])
            trans = ops[CH:]
            state = state + pltpu.roll(state, CH, 1)
            trans = trans + pltpu.roll(trans, CH, 1) + decay_s[i]
            sent = jnp.where(left_half, trans, state).astype(BF16)
            comb[h, :CH, :] = sent
            missed = jnp.where(diag, trans - sent.astype(F32), 0.0)
            comb[h, CH:, :] = jnp.broadcast_to(
                jnp.sum(missed, axis=0, keepdims=True), (EXTRA, TOK)
            ).astype(BF16)

    def group_read(base):
        for i in range(BATCH):
            h = base + i
            rows = slice(h * CH, (h + 1) * CH)
            pread = beside(jnp.where(row <= col, pread_s[h], 0.0))
            kread = beside(jnp.where(row <= col, kread_s[h], 0.0))
            out = fold(mm(solved_s[h], wide(pread)))
            local[h] = out[:CH] + fold(mm(v_ref[rows, :], kread))
            read[h] = jnp.concatenate(halves(out[CH:] + recv_s[h]), axis=0)
            kf = k_ref[rows, :].astype(F32)
            vf = v_ref[rows, :].astype(F32)
            rf = r_ref[rows, :].astype(F32)
            bonus = jnp.sum(rf * kf * par[1, rows, :], axis=0, keepdims=True) * vf
            rest[h] = bonus + par[3, rows, :]

    def comb_copy(h):
        return pltpu.make_async_remote_copy(
            src_ref=comb.at[h],
            dst_ref=inbox.at[me],
            send_sem=comb_send.at[h],
            recv_sem=comb_recv.at[me],
            device_id=(head, owner_of(h)),
            device_id_type=MESH,
        )

    def send_comb(t, carry):
        h = (t // BATCH) * BATCH + (t + me + 3 * (me // 8)) % BATCH

        @pl.when(owner_of(h) != me)
        def _():
            comb_copy(h).start()

        @pl.when(owner_of(h) == me)
        def _():
            inbox[me] = comb[h]

        return carry

    for base in range(0, HEADS, BATCH):
        group_local(base)
        if base == 0:
            pl.semaphore_wait(barrier, SLABS - 1 + 3)
        lax.fori_loop(base, base + BATCH, send_comb, 0)
    for copy in second:
        copy.wait()
    spread(1, rc_ref)
    spread(2, gm_ref)
    spread(3, gb_ref)
    for base in range(0, HEADS, BATCH):
        group_read(base)

    my_y, my_x = me // 8, (me // 2) % 4
    my_head = ((my_x + my_y) % 2) * 8 + 2 * my_y + my_x // 2

    def state_copy(i):
        return pltpu.make_async_remote_copy(
            src_ref=outbox.at[i],
            dst_ref=entering.at[my_head],
            send_sem=state_send.at[i],
            recv_sem=state_recv.at[my_head],
            device_id=(head, i),
            device_id_type=MESH,
        )

    @pl.when(owner_of(my_head) == me)
    def _():
        def arrive(d, carry):
            i = lax.rem(me + d, SLABS)
            pltpu.make_async_remote_copy(
                src_ref=comb.at[0],
                dst_ref=inbox.at[i],
                send_sem=comb_send.at[0],
                recv_sem=comb_recv.at[i],
                device_id=(head, i),
                device_id_type=MESH,
            ).wait_recv()
            return carry

        lax.fori_loop(1, SLABS, arrive, 0)

        def pack(i, value):
            value = value.astype(BF16)
            outbox[i] = jnp.concatenate([value[: CH // 2], value[CH // 2 :]], axis=1)

        def item_of(i):
            item = inbox[i]
            trans = item[:CH, :CH]
            state = pltpu.roll(item[:CH].astype(F32), CH, 1)[:, :CH]
            return trans, item[CH : CH + 1, :CH].astype(F32), state

        groups = SLABS // GROUP
        for g in range(groups):
            trans, missed, state = item_of(g * GROUP)
            whole = trans.astype(F32) + jnp.where(diag[:, :CH], missed, 0.0)
            prefix[g * GROUP] = jnp.concatenate([state, whole], axis=0)

        def step(i, carry):
            for g in range(groups):
                trans, missed, state = item_of(g * GROUP + i)
                old = prefix[g * GROUP + i - 1]
                high, low = halves(old)
                moved = mm(high, trans) + mm(low, trans) + old * missed
                prefix[g * GROUP + i, :CH, :] = moved[:CH] + state
                prefix[g * GROUP + i, CH:, :] = moved[CH:]
            return carry

        lax.fori_loop(1, GROUP, step, 0)
        start = jnp.zeros((CH, CH), F32)
        starts = [start]
        for g in range(groups - 1):
            done = prefix[g * GROUP + GROUP - 1]
            start = dot(start, done[CH:]) + done[:CH]
            starts.append(start)
        for g in range(groups):
            pack(g * GROUP, starts[g])
            for i in range(1, GROUP):
                done = prefix[g * GROUP + i - 1]
                pack(g * GROUP + i, dot(starts[g], done[CH:]) + done[:CH])

        for _, dy, dx, dz in sorted(
            (-min(dy, 4 - dy) - min(dx, 4 - dx) - dz, dy, dx, dz)
            for dy in range(4)
            for dx in range(4)
            for dz in range(2)
            if dy + dx + dz
        ):
            state_copy((my_y + dy) % 4 * 8 + (my_x + dx) % 4 * 2 + (me + dz) % 2).start()
        entering[my_head] = outbox[me]

    def arrived(h):
        @pl.when(owner_of(h) != me)
        def _():
            pltpu.make_async_remote_copy(
                src_ref=outbox.at[0],
                dst_ref=entering.at[h],
                send_sem=state_send.at[0],
                recv_sem=state_recv.at[h],
                device_id=(head, owner_of(h)),
                device_id_type=MESH,
            ).wait_recv()

    for base in range(0, HEADS, BATCH):
        for i in range(BATCH):
            arrived(base + i)
        outs = []
        for i in range(BATCH):
            reading = read[base + i]
            state = entering[base + i]
            nil = jnp.zeros((CH, TOK), BF16)
            upper = jnp.concatenate([reading[:CH], nil, reading[CH:], nil], axis=0)
            lower = jnp.concatenate([nil, reading[:CH], nil, reading[CH:]], axis=0)
            y = mm(
                jnp.concatenate([state, state], axis=1),
                jnp.concatenate([upper, lower], axis=1),
            )
            outs.append(jnp.concatenate([y[:, :TOK], y[:, TOK:]], axis=0) + local[base + i])
        for i in range(BATCH):
            rows = slice((base + i) * CH, (base + i + 1) * CH)
            y = outs[i]
            centred = y - jnp.mean(y, axis=0, keepdims=True)
            spreading = jnp.mean(centred * centred, axis=0, keepdims=True)
            normed = centred * lax.rsqrt(spreading + 0.00064) * par[2, rows, :]
            mixed[rows, :] = ((normed + rest[base + i]) * g_ref[rows, :].astype(F32)).astype(BF16)

    wt_copy.wait()
    partner = pair * 2 + 1 - core
    across = (1 - pair) * 2 + core

    def piece(dest, c):
        rows = pl.ds(pl.multiple_of(dest * ROWS + c * CHUNK, CHUNK), CHUNK)
        return dot(weights[rows, :], mixed[...], precision=None)

    pieces = ROWS // CHUNK

    def near_copy(c):
        return pltpu.make_async_remote_copy(
            src_ref=send_a.at[c],
            dst_ref=got_a.at[c],
            send_sem=rs_send.at[c],
            recv_sem=rs_recv.at[c],
            device_id=(partner, me),
            device_id_type=MESH,
        )

    def far_copy(c):
        return pltpu.make_async_remote_copy(
            src_ref=send_b.at[c],
            dst_ref=got_b.at[c],
            send_sem=rs_send.at[2 * pieces + c],
            recv_sem=rs_recv.at[2 * pieces + c],
            device_id=(across, me),
            device_id_type=MESH,
        )

    for c in range(pieces):
        send_a[c] = piece((1 - pair) * 2 + 1 - core, c)
        near_copy(c).start()
    for c in range(pieces):
        held_b[c] = piece(across, c)
        near_copy(c).wait_recv()
        send_b[c] = (held_b[c] + got_a[c]).astype(BF16)
        far_copy(c).start()
    for c in range(pieces):
        send_a[pieces + c] = piece(partner, c)
        near_copy(pieces + c).start()
    for c in range(pieces):
        rows = slice(c * CHUNK, (c + 1) * CHUNK)
        total[rows, :] = piece(head, c) + skip_ref[rows, :].astype(F32)
        near_copy(pieces + c).wait_recv()
        total[rows, :] = total[rows, :] + got_a[pieces + c]
    for c in range(pieces):
        rows = slice(c * CHUNK, (c + 1) * CHUNK)
        far_copy(c).wait_recv()
        out_ref[rows, :] = (total[rows, :] + got_b[c].astype(F32)).astype(BF16)

    for c in range(2 * pieces):
        near_copy(c).wait_send()
    for c in range(pieces):
        far_copy(c).wait_send()

    def sent_comb(h, carry):
        @pl.when(owner_of(h) != me)
        def _():
            comb_copy(h).wait_send()

        return carry

    lax.fori_loop(0, HEADS, sent_comb, 0)

    @pl.when(owner_of(my_head) == me)
    def _():
        def sent_state(d, carry):
            state_copy(lax.rem(me + d, SLABS)).wait_send()
            return carry

        lax.fori_loop(1, SLABS, sent_state, 0)


def on_device(skip, r, k, v, g, w, a, ef, rc, gm, gb, wt):
    vmem = pl.BlockSpec(memory_space=pltpu.VMEM)
    pieces = ROWS // CHUNK
    dma = pltpu.SemaphoreType.DMA
    return pl.pallas_call(
        kernel,
        out_shape=jax.ShapeDtypeStruct((ROWS, TOK), BF16),
        in_specs=[pl.BlockSpec(memory_space=pltpu.HBM)] * 12,
        out_specs=vmem,
        scratch_shapes=[pltpu.VMEM((ROWS, TOK), BF16)] * 7
        + [pltpu.VMEM((8, 128), F32)] * 4
        + [
            pltpu.VMEM((4, ROWS, TOK), F32),
            pltpu.VMEM((HEADS, CH + EXTRA, 2 * CH), BF16),
            pltpu.VMEM((HEADS, 2 * CH, TOK), BF16),
            pltpu.VMEM((HEADS, CH, TOK), F32),
            pltpu.VMEM((SLABS, CH + EXTRA, 2 * CH), BF16),
            pltpu.VMEM((SLABS, 2 * CH, CH), F32),
            pltpu.VMEM((SLABS, CH // 2, 2 * CH), BF16),
            pltpu.VMEM((HEADS, CH // 2, 2 * CH), BF16),
            pltpu.VMEM((ROWS, TOK), BF16),
            pltpu.VMEM((4 * ROWS, ROWS), BF16),
            pltpu.VMEM((2 * pieces, CHUNK, TOK), F32),
            pltpu.VMEM((2 * pieces, CHUNK, TOK), F32),
            pltpu.VMEM((pieces, CHUNK, TOK), F32),
            pltpu.VMEM((pieces, CHUNK, TOK), BF16),
            pltpu.VMEM((pieces, CHUNK, TOK), BF16),
            pltpu.VMEM((ROWS, TOK), F32),
            pltpu.VMEM((7, TOK, TOK), BF16),
            pltpu.VMEM((BATCH, TOK, TOK), BF16),
            pltpu.VMEM((BATCH, TOK, TOK), BF16),
            pltpu.VMEM((BATCH, TOK, 2 * TOK), BF16),
            pltpu.VMEM((BATCH, TOK, 2 * TOK), BF16),
            pltpu.VMEM((BATCH, TOK, 2 * TOK), BF16),
            pltpu.VMEM((HEADS, TOK, TOK), F32),
            pltpu.VMEM((HEADS, TOK, TOK), F32),
            pltpu.VMEM((BATCH, TOK, 2 * TOK), BF16),
            pltpu.VMEM((BATCH, TOK, TOK), F32),
            pltpu.VMEM((BATCH, TOK, 2 * TOK), BF16),
            pltpu.VMEM((BATCH, TOK, TOK), F32),
            pltpu.VMEM((HEADS, CH, TOK), F32),
            pltpu.VMEM((BATCH, CH, TOK), F32),
            pltpu.VMEM((HEADS, TOK, 2 * TOK), BF16),
            pltpu.VMEM((HEADS, CH, TOK), F32),
            dma((11,)),
            dma(()),
            dma((HEADS,)),
            dma((SLABS,)),
            dma((SLABS,)),
            dma((HEADS,)),
            dma((3 * pieces,)),
            dma((3 * pieces,)),
        ],
        compiler_params=pltpu.CompilerParams(
            collective_id=0, has_side_effects=True, vmem_limit_bytes=40 * 1024 * 1024
        ),
    )(*(
        pltpu.with_memory_space_constraint(x, pltpu.HBM) for x in (skip, r, k, v, g, w, a, *(p.reshape(8, 128) for p in (ef, rc, gm, gb)), wt)
    ))


def solution(mesh):
    split = P("head", "seq")
    vec = P("head")
    return jax.shard_map(
        on_device,
        mesh=mesh,
        in_specs=(split,) * 7 + (vec,) * 4 + (P(None, "head"),),
        out_specs=split,
        check_vma=False,
    )
```

```python
import functools
import jax
import jax.numpy as jnp
from jax import lax
from jax.experimental import pallas as pl
from jax.experimental.pallas import tpu as pltpu
from jax.sharding import PartitionSpec as P

MESH = pl.DeviceIdType.MESH
CH = 64
HEADS = 16
TOK = 128
SLABS = 32
ROWS = 1024
EXTRA = 16
GROUP = 8
BATCH = 8
CHUNK = 256
F32 = jnp.float32
BF16 = jnp.bfloat16


def halves(x):
    high = x.astype(BF16)
    return high, (x - high.astype(F32)).astype(BF16)


def fold(x):
    return x[:, :TOK] + x[:, TOK:]


def mm(left, right):
    return jnp.dot(left, right, preferred_element_type=F32)


def kernel(
    skip_hbm, r_hbm, k_hbm, v_hbm, g_hbm, w_hbm, a_hbm, ef_hbm, rc_hbm, gm_hbm, gb_hbm, wt_hbm,
    out_ref,
    skip_ref, r_ref, k_ref, v_ref, g_ref, w_ref, a_ref, ef_ref, rc_ref, gm_ref, gb_ref,
    par, comb, read, local, inbox, prefix, outbox, entering, mixed, weights,
    send_a, got_a, held_b, send_b, got_b, total,
    masks, pull_t, key_t, ends_t, ahead_s, pair_s, pread_s, kread_s, inv_s, inv, part_s, seen_s,
    recv_s, decay_s, solved_s, rest, pair, both,
    in_sem, wt_sem, comb_send, comb_recv, state_send, state_recv, rs_send, rs_recv,
):
    head = lax.axis_index("head")
    me = lax.axis_index("seq")
    core = lax.rem(head, 2)
    chip = head // 2

    def owner_of(h):
        odd, place = h // 8, h % 8
        y = place // 2
        x = 2 * (place % 2) + (y + odd) % 2
        return y * 8 + x * 2 + (odd + core) % 2

    first = ((ef_hbm, ef_ref), (w_hbm, w_ref), (k_hbm, k_ref), (a_hbm, a_ref), (r_hbm, r_ref), (v_hbm, v_ref))
    second = ((rc_hbm, rc_ref), (gm_hbm, gm_ref), (gb_hbm, gb_ref), (g_hbm, g_ref), (skip_hbm, skip_ref))
    first = [pltpu.make_async_copy(*pair, in_sem.at[n]) for n, pair in enumerate(first)]
    second = [pltpu.make_async_copy(*pair, in_sem.at[6 + n]) for n, pair in enumerate(second)]
    wt_copy = pltpu.make_async_copy(wt_hbm, weights, wt_sem)
    for copy in first + second + [wt_copy]:
        copy.start()

    barrier = pltpu.get_barrier_semaphore()

    def greet(d, carry):
        pl.semaphore_signal(
            barrier, inc=1, device_id=(head, lax.rem(me + d, SLABS)), device_id_type=MESH
        )
        return carry

    lax.fori_loop(1, SLABS, greet, 0)

    def greet_head(d, carry):
        pl.semaphore_signal(
            barrier, inc=1, device_id=(lax.rem(head + d, 4), me), device_id_type=MESH
        )
        return carry

    lax.fori_loop(1, 4, greet_head, 0)

    def spread(p, ref):
        for j in range(8):
            par[p, j * 128 : (j + 1) * 128, :] = jnp.broadcast_to(ref[j : j + 1, :], (128, 128)).T

    for copy in first:
        copy.wait()
    spread(0, ef_ref)

    row = lax.broadcasted_iota(jnp.int32, (TOK, TOK), 0)
    col = lax.broadcasted_iota(jnp.int32, (TOK, TOK), 1)
    upto = jnp.where(row <= col, 1.0, 0.0).astype(BF16)
    apart = row ^ col
    near = (apart >= 2) & (apart < 16)
    masks[...] = jnp.where(apart >= 16, 1.0, 0.0).astype(BF16)
    zero = jnp.zeros((TOK, TOK), BF16)
    diag = lax.broadcasted_iota(jnp.int32, (CH, TOK), 0) == lax.broadcasted_iota(
        jnp.int32, (CH, TOK), 1
    )
    left_half = lax.broadcasted_iota(jnp.int32, (CH, TOK), 1) < CH

    def wide(pair):
        return jnp.concatenate(
            [
                jnp.concatenate([pair[:, :TOK], pair[:, TOK:]], axis=1),
                jnp.concatenate([pair[:, :TOK], zero], axis=1),
            ],
            axis=0,
        )

    def beside(x):
        return jnp.concatenate(halves(x), axis=1)

    def turned(x):
        return jnp.concatenate(halves(x), axis=0).T

    def two_diag(one, other):
        return jnp.concatenate(
            [jnp.concatenate([one, zero], axis=1), jnp.concatenate([zero, other], axis=1)], axis=0
        )

    def group_local(base):
        for i in range(BATCH):
            rows = slice((base + i) * CH, (base + i + 1) * CH)
            w16 = w_ref[rows, :]
            running = mm(w16, upto)
            kf = k_ref[rows, :].astype(F32)
            scaled = kf * par[0, rows, :]
            removal = scaled * lax.rsqrt(jnp.sum(scaled * scaled, axis=0, keepdims=True) + 1e-6)
            pulled = removal * a_ref[rows, :].astype(F32)
            mid = running[:, 63:64]
            end = running[:, 127:128]
            back = jnp.exp(mid - running)
            at_mid = jnp.exp(mid)
            to_end = back * jnp.exp(end - mid)
            removal_fwd = -removal * jnp.exp(running - w16.astype(F32) - mid)
            recept_fwd = r_ref[rows, :].astype(F32) * jnp.exp(running - mid)
            pull_t[i] = turned(pulled * back)
            key_t[i] = turned(kf * back)
            ends_t[i, :, :TOK] = turned(pulled * to_end)
            ends_t[i, :, TOK:] = turned(kf * to_end)
            rem_hi, rem_lo = halves(removal_fwd)
            rec_hi, rec_lo = halves(recept_fwd)
            ahead_s[i, :CH, :TOK] = rem_hi
            ahead_s[i, CH:, :TOK] = rem_lo
            ahead_s[i, :CH, TOK:] = rec_hi
            ahead_s[i, CH:, TOK:] = rec_lo
            seen_s[i, CH:, :] = removal_fwd * at_mid
            recv_s[base + i] = recept_fwd * at_mid
            decay_s[i] = jnp.where(diag, jnp.exp(end), 0.0)
        for i in range(BATCH):
            ahead = ahead_s[i]
            ahead = jnp.concatenate([ahead[:CH], ahead[:CH], ahead[CH:], ahead[CH:]], axis=0)
            pull = pull_t[i]
            from_pull = mm(jnp.concatenate([pull, pull], axis=1), ahead)
            pair_mix = jnp.where(row < col, from_pull[:, :TOK], 0.0)
            pair[i] = pair_mix
            pair_s[i] = beside(pair_mix)
            start = jnp.where(apart == 1, pair_mix, 0.0)
            inv[i] = start
            both[i, TOK:, :TOK] = start.astype(BF16)
            both[i, :TOK, :TOK] = jnp.where(near, pair_mix, 0.0).astype(BF16)
            pread_s[base + i] = from_pull[:, TOK:]
            key = key_t[i]
            from_key = mm(jnp.concatenate([key, key], axis=1), ahead)
            kread_s[base + i] = from_key[:, TOK:]
            part_s[i] = beside(jnp.where(row < col, from_key[:, :TOK], 0.0))
        for i in range(BATCH):
            rows = slice((base + i) * CH, (base + i + 1) * CH)
            seen_s[i, :CH, :] = fold(mm(v_ref[rows, :], part_s[i]))
        for i in range(0, BATCH, 2):
            res = mm(
                jnp.concatenate([both[i, :TOK, :TOK], both[i + 1, :TOK, :TOK]], axis=1),
                two_diag(both[i, TOK:, :TOK], both[i + 1, TOK:, :TOK]),
            )
            for n in range(2):
                e = jnp.where(near, pair[i + n], 0.0) + res[:, n * TOK : (n + 1) * TOK]
                both[i + n, :TOK, :TOK] = e.astype(BF16)
                inv[i + n] = inv[i + n] + e
        for _ in range(2):
            for i in range(0, BATCH, 2):
                res = mm(
                    jnp.concatenate([both[i, :, :TOK], both[i + 1, :, :TOK]], axis=1),
                    two_diag(both[i, :TOK, :TOK], both[i + 1, :TOK, :TOK]),
                )
                for n in range(2):
                    e = res[:TOK, n * TOK : (n + 1) * TOK]
                    m = inv[i + n] + res[TOK:, n * TOK : (n + 1) * TOK]
                    both[i + n, :TOK, :TOK] = e.astype(BF16)
                    both[i + n, TOK:, :TOK] = m.astype(BF16)
                    inv[i + n] = m + e
        for i in range(0, BATCH, 2):
            res = mm(
                jnp.concatenate([both[i, TOK:, :TOK], both[i + 1, TOK:, :TOK]], axis=1),
                two_diag(both[i, :TOK, :TOK], both[i + 1, :TOK, :TOK]),
            )
            for n in range(2):
                whole = jnp.where(row == col, 1.0, inv[i + n] + res[:, n * TOK : (n + 1) * TOK])
                inv_s[i + n] = beside(whole)
        for i in range(BATCH):
            left = jnp.concatenate(
                [pair_s[i] * jnp.concatenate([masks[...], masks[...]], axis=1), beside(seen_s[i])],
                axis=0,
            )
            res = fold(mm(left, wide(inv_s[i])))
            both[i] = beside(res)
            inv[i] = res[TOK:]
        for _ in range(2):
            for i in range(BATCH):
                res = fold(mm(both[i], wide(both[i, :TOK, :])))
                g = inv[i] + res[TOK:]
                both[i, :TOK, :] = beside(res[:TOK])
                both[i, TOK:, :] = beside(g)
                inv[i] = g
        for i in range(BATCH):
            solved_s[base + i] = beside(
                inv[i] + fold(mm(both[i, TOK:, :], wide(both[i, :TOK, :])))
            )
        for i in range(BATCH):
            h = base + i
            rows = slice(h * CH, (h + 1) * CH)
            pull_end = ends_t[i, :, :TOK]
            ops = mm(solved_s[h], jnp.concatenate([pull_end, pull_end], axis=0))
            state = ops[:CH] + mm(v_ref[rows, :], ends_t[i, :, TOK:])
            trans = ops[CH:]
            state = state + pltpu.roll(state, CH, 1)
            trans = trans + pltpu.roll(trans, CH, 1) + decay_s[i]
            sent = jnp.where(left_half, trans, state).astype(BF16)
            comb[h, :CH, :] = sent
            missed = jnp.where(diag, trans - sent.astype(F32), 0.0)
            comb[h, CH:, :] = jnp.broadcast_to(
                jnp.sum(missed, axis=0, keepdims=True), (EXTRA, TOK)
            ).astype(BF16)

    def group_read(base):
        for i in range(BATCH):
            h = base + i
            rows = slice(h * CH, (h + 1) * CH)
            pread = beside(jnp.where(row <= col, pread_s[h], 0.0))
            kread = beside(jnp.where(row <= col, kread_s[h], 0.0))
            out = fold(mm(solved_s[h], wide(pread)))
            local[h] = out[:CH] + fold(mm(v_ref[rows, :], kread))
            read[h] = jnp.concatenate(halves(out[CH:] + recv_s[h]), axis=0)
            kf = k_ref[rows, :].astype(F32)
            vf = v_ref[rows, :].astype(F32)
            rf = r_ref[rows, :].astype(F32)
            bonus = jnp.sum(rf * kf * par[1, rows, :], axis=0, keepdims=True) * vf
            rest[h] = bonus + par[3, rows, :]

    def comb_copy(h):
        return pltpu.make_async_remote_copy(
            src_ref=comb.at[h],
            dst_ref=inbox.at[me],
            send_sem=comb_send.at[h],
            recv_sem=comb_recv.at[me],
            device_id=(head, owner_of(h)),
            device_id_type=MESH,
        )

    def send_comb(t, carry):
        h = (t // BATCH) * BATCH + (t + me + 3 * (me // 8)) % BATCH

        @pl.when(owner_of(h) != me)
        def _():
            comb_copy(h).start()

        @pl.when(owner_of(h) == me)
        def _():
            inbox[me] = comb[h]

        return carry

    for base in range(0, HEADS, BATCH):
        group_local(base)
        if base == 0:
            pl.semaphore_wait(barrier, SLABS - 1 + 3)
        lax.fori_loop(base, base + BATCH, send_comb, 0)
    for copy in second:
        copy.wait()
    spread(1, rc_ref)
    spread(2, gm_ref)
    spread(3, gb_ref)
    for base in range(0, HEADS, BATCH):
        group_read(base)

    my_y, my_x = me // 8, (me // 2) % 4
    my_head = ((my_x + my_y) % 2) * 8 + 2 * my_y + my_x // 2

    def state_copy(i):
        return pltpu.make_async_remote_copy(
            src_ref=outbox.at[i],
            dst_ref=entering.at[my_head],
            send_sem=state_send.at[i],
            recv_sem=state_recv.at[my_head],
            device_id=(head, i),
            device_id_type=MESH,
        )

    @pl.when(owner_of(my_head) == me)
    def _():
        def arrive(d, carry):
            i = lax.rem(me + d, SLABS)
            pltpu.make_async_remote_copy(
                src_ref=comb.at[0],
                dst_ref=inbox.at[i],
                send_sem=comb_send.at[0],
                recv_sem=comb_recv.at[i],
                device_id=(head, i),
                device_id_type=MESH,
            ).wait_recv()
            return carry

        lax.fori_loop(1, SLABS, arrive, 0)

        def pack(i, value):
            half = CH // 2
            outbox[i] = jnp.where(left_half[:half], value[:half], value[half:]).astype(BF16)

        def item_of(i):
            item = inbox[i].astype(F32)
            swapped = pltpu.roll(item, CH, 1)
            trans = jnp.where(left_half, item[:CH], swapped[:CH])
            state = jnp.where(left_half, swapped[:CH], item[:CH])
            missed = jnp.where(left_half[:1], item[CH : CH + 1], swapped[CH : CH + 1])
            return trans, missed, state

        def left_of(x):
            return jnp.where(wide_half[: x.shape[0]], x, x - x.astype(BF16).astype(F32)).astype(BF16)

        def right_of(x):
            high, low = halves(x)
            none = jnp.zeros((CH, TOK), BF16)
            return jnp.concatenate(
                [jnp.concatenate([high, low], axis=1), jnp.concatenate([high, none], axis=1)],
                axis=0,
            )

        wide_half = lax.broadcasted_iota(jnp.int32, (TOK, TOK), 1) < CH
        groups = SLABS // GROUP
        for g in range(groups):
            trans, missed, state = item_of(g * GROUP)
            prefix[g * GROUP, :CH, :] = state
            prefix[g * GROUP, CH:, :] = trans + jnp.where((row % CH == col % CH)[:CH], missed, 0.0)

        def step(i, carry):
            for g in range(groups):
                trans, missed, state = item_of(g * GROUP + i)
                trans = trans.astype(BF16)
                old = prefix[g * GROUP + i - 1]
                moved = mm(left_of(old), jnp.concatenate([trans, trans], axis=0)) + old * missed
                prefix[g * GROUP + i, :CH, :] = moved[:CH] + state
                prefix[g * GROUP + i, CH:, :] = moved[CH:]
            return carry

        lax.fori_loop(1, GROUP, step, 0)
        start = jnp.zeros((CH, TOK), F32)
        starts = [start]
        for g in range(groups - 1):
            done = prefix[g * GROUP + GROUP - 1]
            start = done[:CH] if g == 0 else fold(mm(left_of(start), right_of(done[CH:]))) + done[:CH]
            starts.append(start)
        for g in range(groups):
            pack(g * GROUP, starts[g])
            for i in range(1, GROUP):
                done = prefix[g * GROUP + i - 1]
                moved = fold(mm(left_of(starts[g]), right_of(done[CH:]))) if g else 0.0
                pack(g * GROUP + i, moved + done[:CH])

        for _, dy, dx, dz in sorted(
            (-min(dy, 4 - dy) - min(dx, 4 - dx) - dz, dy, dx, dz)
            for dy in range(4)
            for dx in range(4)
            for dz in range(2)
            if dy + dx + dz
        ):
            state_copy((my_y + dy) % 4 * 8 + (my_x + dx) % 4 * 2 + (me + dz) % 2).start()
        entering[my_head] = outbox[me]

    def arrived(h):
        @pl.when(owner_of(h) != me)
        def _():
            pltpu.make_async_remote_copy(
                src_ref=outbox.at[0],
                dst_ref=entering.at[h],
                send_sem=state_send.at[0],
                recv_sem=state_recv.at[h],
                device_id=(head, owner_of(h)),
                device_id_type=MESH,
            ).wait_recv()

    for base in range(0, HEADS, BATCH):
        for i in range(BATCH):
            arrived(base + i)
        outs = []
        for i in range(BATCH):
            reading = read[base + i]
            state = entering[base + i]
            nil = jnp.zeros((CH, TOK), BF16)
            upper = jnp.concatenate([reading[:CH], nil, reading[CH:], nil], axis=0)
            lower = jnp.concatenate([nil, reading[:CH], nil, reading[CH:]], axis=0)
            y = mm(
                jnp.concatenate([state, state], axis=1),
                jnp.concatenate([upper, lower], axis=1),
            )
            outs.append(jnp.concatenate([y[:, :TOK], y[:, TOK:]], axis=0) + local[base + i])
        for i in range(BATCH):
            rows = slice((base + i) * CH, (base + i + 1) * CH)
            y = outs[i]
            centred = y - jnp.mean(y, axis=0, keepdims=True)
            spreading = jnp.mean(centred * centred, axis=0, keepdims=True)
            normed = centred * lax.rsqrt(spreading + 0.00064) * par[2, rows, :]
            mixed[rows, :] = ((normed + rest[base + i]) * g_ref[rows, :].astype(F32)).astype(BF16)

    wt_copy.wait()
    partner = chip * 2 + 1 - core
    across = (1 - chip) * 2 + core

    def piece(dest, c):
        rows = pl.ds(pl.multiple_of(dest * ROWS + c * CHUNK, CHUNK), CHUNK)
        return mm(weights[rows, :], mixed[...])

    pieces = ROWS // CHUNK

    def near_copy(c):
        return pltpu.make_async_remote_copy(
            src_ref=send_a.at[c],
            dst_ref=got_a.at[c],
            send_sem=rs_send.at[c],
            recv_sem=rs_recv.at[c],
            device_id=(partner, me),
            device_id_type=MESH,
        )

    def far_copy(c):
        return pltpu.make_async_remote_copy(
            src_ref=send_b.at[c],
            dst_ref=got_b.at[c],
            send_sem=rs_send.at[2 * pieces + c],
            recv_sem=rs_recv.at[2 * pieces + c],
            device_id=(across, me),
            device_id_type=MESH,
        )

    for c in range(pieces):
        send_a[c] = piece((1 - chip) * 2 + 1 - core, c)
        near_copy(c).start()
    for c in range(pieces):
        held_b[c] = piece(across, c)
        near_copy(c).wait_recv()
        send_b[c] = (held_b[c] + got_a[c]).astype(BF16)
        far_copy(c).start()
    for c in range(pieces):
        send_a[pieces + c] = piece(partner, c)
        near_copy(pieces + c).start()
    for c in range(pieces):
        rows = slice(c * CHUNK, (c + 1) * CHUNK)
        total[rows, :] = piece(head, c) + skip_ref[rows, :].astype(F32)
        near_copy(pieces + c).wait_recv()
        total[rows, :] = total[rows, :] + got_a[pieces + c]
    for c in range(pieces):
        rows = slice(c * CHUNK, (c + 1) * CHUNK)
        far_copy(c).wait_recv()
        out_ref[rows, :] = (total[rows, :] + got_b[c].astype(F32)).astype(BF16)

    for c in range(2 * pieces):
        near_copy(c).wait_send()
    for c in range(pieces):
        far_copy(c).wait_send()

    def sent_comb(h, carry):
        @pl.when(owner_of(h) != me)
        def _():
            comb_copy(h).wait_send()

        return carry

    lax.fori_loop(0, HEADS, sent_comb, 0)

    @pl.when(owner_of(my_head) == me)
    def _():
        def sent_state(d, carry):
            state_copy(lax.rem(me + d, SLABS)).wait_send()
            return carry

        lax.fori_loop(1, SLABS, sent_state, 0)


def on_device(skip, r, k, v, g, w, a, ef, rc, gm, gb, wt):
    vmem = pl.BlockSpec(memory_space=pltpu.VMEM)
    pieces = ROWS // CHUNK
    dma = pltpu.SemaphoreType.DMA
    return pl.pallas_call(
        kernel,
        out_shape=jax.ShapeDtypeStruct((ROWS, TOK), BF16),
        in_specs=[pl.BlockSpec(memory_space=pltpu.HBM)] * 12,
        out_specs=vmem,
        scratch_shapes=[pltpu.VMEM((ROWS, TOK), BF16)] * 7
        + [pltpu.VMEM((8, 128), F32)] * 4
        + [
            pltpu.VMEM((4, ROWS, TOK), F32),
            pltpu.VMEM((HEADS, CH + EXTRA, 2 * CH), BF16),
            pltpu.VMEM((HEADS, 2 * CH, TOK), BF16),
            pltpu.VMEM((HEADS, CH, TOK), F32),
            pltpu.VMEM((SLABS, CH + EXTRA, 2 * CH), BF16),
            pltpu.VMEM((SLABS, TOK, TOK), F32),
            pltpu.VMEM((SLABS, CH // 2, 2 * CH), BF16),
            pltpu.VMEM((HEADS, CH // 2, 2 * CH), BF16),
            pltpu.VMEM((ROWS, TOK), BF16),
            pltpu.VMEM((4 * ROWS, ROWS), BF16),
            pltpu.VMEM((2 * pieces, CHUNK, TOK), F32),
            pltpu.VMEM((2 * pieces, CHUNK, TOK), F32),
            pltpu.VMEM((pieces, CHUNK, TOK), F32),
            pltpu.VMEM((pieces, CHUNK, TOK), BF16),
            pltpu.VMEM((pieces, CHUNK, TOK), BF16),
            pltpu.VMEM((ROWS, TOK), F32),
            pltpu.VMEM((TOK, TOK), BF16),
            pltpu.VMEM((BATCH, TOK, TOK), BF16),
            pltpu.VMEM((BATCH, TOK, TOK), BF16),
            pltpu.VMEM((BATCH, TOK, 2 * TOK), BF16),
            pltpu.VMEM((BATCH, TOK, 2 * TOK), BF16),
            pltpu.VMEM((BATCH, TOK, 2 * TOK), BF16),
            pltpu.VMEM((HEADS, TOK, TOK), F32),
            pltpu.VMEM((HEADS, TOK, TOK), F32),
            pltpu.VMEM((BATCH, TOK, 2 * TOK), BF16),
            pltpu.VMEM((BATCH, TOK, TOK), F32),
            pltpu.VMEM((BATCH, TOK, 2 * TOK), BF16),
            pltpu.VMEM((BATCH, TOK, TOK), F32),
            pltpu.VMEM((HEADS, CH, TOK), F32),
            pltpu.VMEM((BATCH, CH, TOK), F32),
            pltpu.VMEM((HEADS, TOK, 2 * TOK), BF16),
            pltpu.VMEM((HEADS, CH, TOK), F32),
            pltpu.VMEM((BATCH, TOK, TOK), F32),
            pltpu.VMEM((BATCH, 2 * TOK, 2 * TOK), BF16),
            dma((11,)),
            dma(()),
            dma((HEADS,)),
            dma((SLABS,)),
            dma((SLABS,)),
            dma((HEADS,)),
            dma((3 * pieces,)),
            dma((3 * pieces,)),
        ],
        compiler_params=pltpu.CompilerParams(
            collective_id=0, has_side_effects=True, vmem_limit_bytes=40 * 1024 * 1024
        ),
    )(*(
        pltpu.with_memory_space_constraint(x, pltpu.HBM) for x in (skip, r, k, v, g, w, a, *(p.reshape(8, 128) for p in (ef, rc, gm, gb)), wt)
    ))


def solution(mesh):
    split = P("head", "seq")
    vec = P("head")
    return jax.shard_map(
        on_device,
        mesh=mesh,
        in_specs=(split,) * 7 + (vec,) * 4 + (P(None, "head"),),
        out_specs=split,
        check_vma=False,
    )
```

```python
import functools
import jax
import jax.numpy as jnp
from jax import lax
from jax.experimental import pallas as pl
from jax.experimental.pallas import tpu as pltpu
from jax.sharding import PartitionSpec as P

MESH = pl.DeviceIdType.MESH
CH = 64
HEADS = 16
TOK = 128
SLABS = 32
ROWS = 1024
EXTRA = 16
GROUP = 8
BATCH = 8
CHUNK = 128
F32 = jnp.float32
BF16 = jnp.bfloat16


def halves(x):
    high = x.astype(BF16)
    return high, (x - high.astype(F32)).astype(BF16)


def fold(x):
    return x[:, :TOK] + x[:, TOK:]


def mm(left, right):
    return jnp.dot(left, right, preferred_element_type=F32)


def kernel(
    skip_hbm, r_hbm, k_hbm, v_hbm, g_hbm, w_hbm, a_hbm, ef_hbm, rc_hbm, gm_hbm, gb_hbm, wt_hbm,
    out_ref,
    skip_ref, r_ref, k_ref, v_ref, g_ref, w_ref, a_ref, ef_ref, rc_ref, gm_ref, gb_ref,
    par, comb, read, local, inbox, prefix, outbox, entering, mixed, weights,
    send_a, got_a, held_b, send_b, got_b, total,
    pull_t, key_t, ends_t, ahead_s, pair_s, inv_s, inv, part_s, seen_s,
    recv_s, decay_s, solved_s, rest, both,
    in_sem, wt_sem, comb_send, comb_recv, state_send, state_recv, rs_send, rs_recv,
):
    head = lax.axis_index("head")
    me = lax.axis_index("seq")
    core = lax.rem(head, 2)
    chip = head // 2

    def owner_of(h):
        odd, place = h // 8, h % 8
        y = place // 2
        x = 2 * (place % 2) + (y + odd) % 2
        return y * 8 + x * 2 + (odd + core) % 2

    first = ((ef_hbm, ef_ref), (w_hbm, w_ref), (k_hbm, k_ref), (a_hbm, a_ref), (r_hbm, r_ref), (v_hbm, v_ref))
    second = ((rc_hbm, rc_ref), (gm_hbm, gm_ref), (gb_hbm, gb_ref), (g_hbm, g_ref), (skip_hbm, skip_ref))
    first = [pltpu.make_async_copy(*pair, in_sem.at[n]) for n, pair in enumerate(first)]
    second = [pltpu.make_async_copy(*pair, in_sem.at[6 + n]) for n, pair in enumerate(second)]
    wt_copy = pltpu.make_async_copy(wt_hbm, weights, wt_sem)
    for copy in first:
        copy.start()

    barrier = pltpu.get_barrier_semaphore()

    def greet(d, carry):
        pl.semaphore_signal(
            barrier, inc=1, device_id=(head, lax.rem(me + d, SLABS)), device_id_type=MESH
        )
        return carry

    lax.fori_loop(1, SLABS, greet, 0)

    def greet_head(d, carry):
        pl.semaphore_signal(
            barrier, inc=1, device_id=(lax.rem(head + d, 4), me), device_id_type=MESH
        )
        return carry

    lax.fori_loop(1, 4, greet_head, 0)

    def spread(p, ref):
        for j in range(8):
            par[p, j * 128 : (j + 1) * 128, :] = jnp.broadcast_to(ref[j : j + 1, :], (128, 128)).T

    for copy in first:
        copy.wait()
    for copy in second + [wt_copy]:
        copy.start()
    spread(0, ef_ref)

    row = lax.broadcasted_iota(jnp.int32, (TOK, TOK), 0)
    col = lax.broadcasted_iota(jnp.int32, (TOK, TOK), 1)
    upto = jnp.where(row <= col, 1.0, 0.0).astype(BF16)
    apart = row ^ col
    near = (apart >= 2) & (apart < 16)
    zero = jnp.zeros((TOK, TOK), BF16)
    diag = lax.broadcasted_iota(jnp.int32, (CH, TOK), 0) == lax.broadcasted_iota(
        jnp.int32, (CH, TOK), 1
    )
    left_half = lax.broadcasted_iota(jnp.int32, (CH, TOK), 1) < CH

    def wide(pair):
        return jnp.concatenate(
            [
                jnp.concatenate([pair[:, :TOK], pair[:, TOK:]], axis=1),
                jnp.concatenate([pair[:, :TOK], zero], axis=1),
            ],
            axis=0,
        )

    def beside(x):
        return jnp.concatenate(halves(x), axis=1)

    def turned(x):
        return jnp.concatenate(halves(x), axis=0).T

    def two_diag(one, other):
        return jnp.concatenate(
            [jnp.concatenate([one, zero], axis=1), jnp.concatenate([zero, other], axis=1)], axis=0
        )

    def group_local(base):
        for i in range(BATCH):
            rows = slice((base + i) * CH, (base + i + 1) * CH)
            w16 = w_ref[rows, :]
            running = mm(w16, upto)
            kf = k_ref[rows, :].astype(F32)
            scaled = kf * par[0, rows, :]
            removal = scaled * lax.rsqrt(jnp.sum(scaled * scaled, axis=0, keepdims=True) + 1e-6)
            pulled = removal * a_ref[rows, :].astype(F32)
            mid = running[:, 63:64]
            end = running[:, 127:128]
            back = jnp.exp(mid - running)
            at_mid = jnp.exp(mid)
            to_end = back * jnp.exp(end - mid)
            removal_fwd = -removal * jnp.exp(running - w16.astype(F32) - mid)
            pull_t[base + i] = turned(pulled * back)
            key_t[base + i] = turned(kf * back)
            ends_t[i, :, :TOK] = turned(pulled * to_end)
            ends_t[i, :, TOK:] = turned(kf * to_end)
            rem_hi, rem_lo = halves(removal_fwd)
            ahead_s[i, :CH, :] = rem_hi
            ahead_s[i, CH:, :] = rem_lo
            seen_s[i, CH:, :] = removal_fwd * at_mid
            decay_s[i] = jnp.where(diag, jnp.exp(end), 0.0)
        for i in range(BATCH):
            ahead = ahead_s[i]
            ahead = jnp.concatenate([ahead[:CH], ahead[:CH], ahead[CH:], ahead[CH:]], axis=0)
            pull = pull_t[base + i]
            from_pull = mm(jnp.concatenate([pull, pull], axis=1), ahead)
            pair_mix = jnp.where(row < col, from_pull, 0.0)
            pair_s[i] = beside(jnp.where(apart >= 16, pair_mix, 0.0))
            inv[i] = jnp.where(apart < 16, pair_mix, 0.0)
            both[i, TOK:, :TOK] = jnp.where(apart == 1, pair_mix, 0.0).astype(BF16)
            both[i, :TOK, :TOK] = jnp.where(near, pair_mix, 0.0).astype(BF16)
            key = key_t[base + i]
            from_key = mm(jnp.concatenate([key, key], axis=1), ahead)
            part_s[i] = beside(jnp.where(row < col, from_key, 0.0))
        for i in range(BATCH):
            rows = slice((base + i) * CH, (base + i + 1) * CH)
            seen_s[i, :CH, :] = fold(mm(v_ref[rows, :], part_s[i]))
        for i in range(0, BATCH, 2):
            res = mm(
                jnp.concatenate([both[i, :TOK, :TOK], both[i + 1, :TOK, :TOK]], axis=1),
                two_diag(both[i, TOK:, :TOK], both[i + 1, TOK:, :TOK]),
            )
            for n in range(2):
                more = res[:, n * TOK : (n + 1) * TOK]
                both[i + n, :TOK, :TOK] = (both[i + n, :TOK, :TOK].astype(F32) + more).astype(BF16)
                inv[i + n] = inv[i + n] + more
        for _ in range(2):
            for i in range(0, BATCH, 2):
                res = mm(
                    jnp.concatenate([both[i, :, :TOK], both[i + 1, :, :TOK]], axis=1),
                    two_diag(both[i, :TOK, :TOK], both[i + 1, :TOK, :TOK]),
                )
                for n in range(2):
                    e = res[:TOK, n * TOK : (n + 1) * TOK]
                    m = inv[i + n] + res[TOK:, n * TOK : (n + 1) * TOK]
                    both[i + n, :TOK, :TOK] = e.astype(BF16)
                    both[i + n, TOK:, :TOK] = m.astype(BF16)
                    inv[i + n] = m + e
        for i in range(0, BATCH, 2):
            res = mm(
                jnp.concatenate([both[i, TOK:, :TOK], both[i + 1, TOK:, :TOK]], axis=1),
                two_diag(both[i, :TOK, :TOK], both[i + 1, :TOK, :TOK]),
            )
            for n in range(2):
                whole = jnp.where(row == col, 1.0, inv[i + n] + res[:, n * TOK : (n + 1) * TOK])
                inv_s[i + n] = beside(whole)
        for i in range(BATCH):
            left = jnp.concatenate([pair_s[i], beside(seen_s[i])], axis=0)
            res = fold(mm(left, wide(inv_s[i])))
            both[i] = beside(res)
            inv[i] = res[TOK:]
        for _ in range(2):
            for i in range(BATCH):
                res = fold(mm(both[i], wide(both[i, :TOK, :])))
                g = inv[i] + res[TOK:]
                both[i, :TOK, :] = beside(res[:TOK])
                both[i, TOK:, :] = beside(g)
                inv[i] = g
        for i in range(BATCH):
            solved_s[base + i] = beside(
                inv[i] + fold(mm(both[i, TOK:, :], wide(both[i, :TOK, :])))
            )
        for i in range(BATCH):
            h = base + i
            rows = slice(h * CH, (h + 1) * CH)
            pull_end = ends_t[i, :, :TOK]
            ops = mm(solved_s[h], jnp.concatenate([pull_end, pull_end], axis=0))
            state = ops[:CH] + mm(v_ref[rows, :], ends_t[i, :, TOK:])
            trans = ops[CH:]
            state = state + pltpu.roll(state, CH, 1)
            trans = trans + pltpu.roll(trans, CH, 1) + decay_s[i]
            sent = jnp.where(left_half, trans, state).astype(BF16)
            comb[h, :CH, :] = sent
            missed = jnp.where(diag, trans - sent.astype(F32), 0.0)
            comb[h, CH:, :] = jnp.broadcast_to(
                jnp.sum(missed, axis=0, keepdims=True), (EXTRA, TOK)
            ).astype(BF16)

    def group_read(base):
        for i in range(BATCH):
            h = base + i
            rows = slice(h * CH, (h + 1) * CH)
            running = mm(w_ref[rows, :], upto)
            mid = running[:, 63:64]
            recept_fwd = r_ref[rows, :].astype(F32) * jnp.exp(running - mid)
            recv_s[i] = recept_fwd * jnp.exp(mid)
            high, low = halves(recept_fwd)
            ahead = jnp.concatenate([high, high, low, low], axis=0)
            pull, key = pull_t[h], key_t[h]
            pread = mm(jnp.concatenate([pull, pull], axis=1), ahead)
            kread = mm(jnp.concatenate([key, key], axis=1), ahead)
            pair_s[i] = beside(jnp.where(row <= col, pread, 0.0))
            part_s[i] = beside(jnp.where(row <= col, kread, 0.0))
        for i in range(BATCH):
            h = base + i
            rows = slice(h * CH, (h + 1) * CH)
            out = fold(mm(solved_s[h], wide(pair_s[i])))
            local[h] = out[:CH] + fold(mm(v_ref[rows, :], part_s[i]))
            read[h] = jnp.concatenate(halves(out[CH:] + recv_s[i]), axis=0)
            kf = k_ref[rows, :].astype(F32)
            vf = v_ref[rows, :].astype(F32)
            rf = r_ref[rows, :].astype(F32)
            bonus = jnp.sum(rf * kf * par[1, rows, :], axis=0, keepdims=True) * vf
            rest[h] = bonus + par[3, rows, :]

    def comb_copy(h):
        return pltpu.make_async_remote_copy(
            src_ref=comb.at[h],
            dst_ref=inbox.at[me],
            send_sem=comb_send.at[h],
            recv_sem=comb_recv.at[me],
            device_id=(head, owner_of(h)),
            device_id_type=MESH,
        )

    def send_comb(t, carry):
        h = (t // BATCH) * BATCH + (t + me + 3 * (me // 8)) % BATCH

        @pl.when(owner_of(h) != me)
        def _():
            comb_copy(h).start()

        @pl.when(owner_of(h) == me)
        def _():
            inbox[me] = comb[h]

        return carry

    for base in range(0, HEADS, BATCH):
        group_local(base)
        if base == 0:
            pl.semaphore_wait(barrier, SLABS - 1 + 3)
        lax.fori_loop(base, base + BATCH, send_comb, 0)
    for copy in second:
        copy.wait()
    spread(1, rc_ref)
    spread(2, gm_ref)
    spread(3, gb_ref)
    for base in range(0, HEADS, BATCH):
        group_read(base)

    my_y, my_x = me // 8, (me // 2) % 4
    my_head = ((my_x + my_y) % 2) * 8 + 2 * my_y + my_x // 2

    def state_copy(i):
        return pltpu.make_async_remote_copy(
            src_ref=outbox.at[i],
            dst_ref=entering.at[my_head],
            send_sem=state_send.at[i],
            recv_sem=state_recv.at[my_head],
            device_id=(head, i),
            device_id_type=MESH,
        )

    @pl.when(owner_of(my_head) == me)
    def _():
        def arrive(d, carry):
            i = lax.rem(me + d, SLABS)
            pltpu.make_async_remote_copy(
                src_ref=comb.at[0],
                dst_ref=inbox.at[i],
                send_sem=comb_send.at[0],
                recv_sem=comb_recv.at[i],
                device_id=(head, i),
                device_id_type=MESH,
            ).wait_recv()
            return carry

        lax.fori_loop(1, SLABS, arrive, 0)

        def pack(i, value):
            half = CH // 2
            outbox[i] = jnp.where(left_half[:half], value[:half], value[half:]).astype(BF16)

        def item_of(i):
            item = inbox[i].astype(F32)
            swapped = pltpu.roll(item, CH, 1)
            trans = jnp.where(left_half, item[:CH], swapped[:CH])
            state = jnp.where(left_half, swapped[:CH], item[:CH])
            missed = jnp.where(left_half[:1], item[CH : CH + 1], swapped[CH : CH + 1])
            return trans, missed, state

        def left_of(x):
            return jnp.where(wide_half[: x.shape[0]], x, x - x.astype(BF16).astype(F32)).astype(BF16)

        def right_of(x):
            high, low = halves(x)
            none = jnp.zeros((CH, TOK), BF16)
            return jnp.concatenate(
                [jnp.concatenate([high, low], axis=1), jnp.concatenate([high, none], axis=1)],
                axis=0,
            )

        wide_half = lax.broadcasted_iota(jnp.int32, (TOK, TOK), 1) < CH
        groups = SLABS // GROUP
        for g in range(groups):
            trans, missed, state = item_of(g * GROUP)
            prefix[g * GROUP, :CH, :] = state
            prefix[g * GROUP, CH:, :] = trans + jnp.where((row % CH == col % CH)[:CH], missed, 0.0)

        def step(i, carry):
            for g in range(groups):
                trans, missed, state = item_of(g * GROUP + i)
                trans = trans.astype(BF16)
                old = prefix[g * GROUP + i - 1]
                moved = mm(left_of(old), jnp.concatenate([trans, trans], axis=0)) + old * missed
                prefix[g * GROUP + i, :CH, :] = moved[:CH] + state
                prefix[g * GROUP + i, CH:, :] = moved[CH:]
            return carry

        lax.fori_loop(1, GROUP, step, 0)
        start = jnp.zeros((CH, TOK), F32)
        starts = [start]
        for g in range(groups - 1):
            done = prefix[g * GROUP + GROUP - 1]
            start = done[:CH] if g == 0 else fold(mm(left_of(start), right_of(done[CH:]))) + done[:CH]
            starts.append(start)
        for g in range(groups):
            pack(g * GROUP, starts[g])
            for i in range(1, GROUP):
                done = prefix[g * GROUP + i - 1]
                moved = fold(mm(left_of(starts[g]), right_of(done[CH:]))) if g else 0.0
                pack(g * GROUP + i, moved + done[:CH])

        for _, dy, dx, dz in sorted(
            (-min(dy, 4 - dy) - min(dx, 4 - dx) - dz, dy, dx, dz)
            for dy in range(4)
            for dx in range(4)
            for dz in range(2)
            if dy + dx + dz
        ):
            state_copy((my_y + dy) % 4 * 8 + (my_x + dx) % 4 * 2 + (me + dz) % 2).start()
        entering[my_head] = outbox[me]

    def arrived(h):
        @pl.when(owner_of(h) != me)
        def _():
            pltpu.make_async_remote_copy(
                src_ref=outbox.at[0],
                dst_ref=entering.at[h],
                send_sem=state_send.at[0],
                recv_sem=state_recv.at[h],
                device_id=(head, owner_of(h)),
                device_id_type=MESH,
            ).wait_recv()

    for base in range(0, HEADS, BATCH):
        for i in range(BATCH):
            arrived(base + i)
        outs = []
        for i in range(BATCH):
            reading = read[base + i]
            state = entering[base + i]
            nil = jnp.zeros((CH, TOK), BF16)
            upper = jnp.concatenate([reading[:CH], nil, reading[CH:], nil], axis=0)
            lower = jnp.concatenate([nil, reading[:CH], nil, reading[CH:]], axis=0)
            y = mm(
                jnp.concatenate([state, state], axis=1),
                jnp.concatenate([upper, lower], axis=1),
            )
            outs.append(jnp.concatenate([y[:, :TOK], y[:, TOK:]], axis=0) + local[base + i])
        for i in range(BATCH):
            rows = slice((base + i) * CH, (base + i + 1) * CH)
            y = outs[i]
            centred = y - jnp.mean(y, axis=0, keepdims=True)
            spreading = jnp.mean(centred * centred, axis=0, keepdims=True)
            normed = centred * lax.rsqrt(spreading + 0.00064) * par[2, rows, :]
            mixed[rows, :] = ((normed + rest[base + i]) * g_ref[rows, :].astype(F32)).astype(BF16)

    wt_copy.wait()
    partner = chip * 2 + 1 - core
    across = (1 - chip) * 2 + core

    def piece(dest, c):
        rows = pl.ds(pl.multiple_of(dest * ROWS + c * CHUNK, CHUNK), CHUNK)
        return mm(weights[rows, :], mixed[...])

    pieces = ROWS // CHUNK

    def near_copy(c):
        return pltpu.make_async_remote_copy(
            src_ref=send_a.at[c],
            dst_ref=got_a.at[c],
            send_sem=rs_send.at[c],
            recv_sem=rs_recv.at[c],
            device_id=(partner, me),
            device_id_type=MESH,
        )

    def far_copy(c):
        return pltpu.make_async_remote_copy(
            src_ref=send_b.at[c],
            dst_ref=got_b.at[c],
            send_sem=rs_send.at[2 * pieces + c],
            recv_sem=rs_recv.at[2 * pieces + c],
            device_id=(across, me),
            device_id_type=MESH,
        )

    for c in range(pieces):
        send_a[c] = piece((1 - chip) * 2 + 1 - core, c)
        near_copy(c).start()
    for c in range(pieces):
        held_b[c] = piece(across, c)
        near_copy(c).wait_recv()
        send_b[c] = (held_b[c] + got_a[c]).astype(BF16)
        far_copy(c).start()
    for c in range(pieces):
        send_a[pieces + c] = piece(partner, c)
        near_copy(pieces + c).start()
    for c in range(pieces):
        rows = slice(c * CHUNK, (c + 1) * CHUNK)
        total[rows, :] = piece(head, c) + skip_ref[rows, :].astype(F32)
        near_copy(pieces + c).wait_recv()
        total[rows, :] = total[rows, :] + got_a[pieces + c]
    for c in range(2 * pieces):
        near_copy(c).wait_send()

    def sent_comb(h, carry):
        @pl.when(owner_of(h) != me)
        def _():
            comb_copy(h).wait_send()

        return carry

    lax.fori_loop(0, HEADS, sent_comb, 0)

    @pl.when(owner_of(my_head) == me)
    def _():
        def sent_state(d, carry):
            state_copy(lax.rem(me + d, SLABS)).wait_send()
            return carry

        lax.fori_loop(1, SLABS, sent_state, 0)

    for c in range(pieces):
        rows = slice(c * CHUNK, (c + 1) * CHUNK)
        far_copy(c).wait_recv()
        out_ref[rows, :] = (total[rows, :] + got_b[c].astype(F32)).astype(BF16)
    for c in range(pieces):
        far_copy(c).wait_send()


def on_device(skip, r, k, v, g, w, a, ef, rc, gm, gb, wt):
    vmem = pl.BlockSpec(memory_space=pltpu.VMEM)
    pieces = ROWS // CHUNK
    dma = pltpu.SemaphoreType.DMA
    return pl.pallas_call(
        kernel,
        out_shape=jax.ShapeDtypeStruct((ROWS, TOK), BF16),
        in_specs=[pl.BlockSpec(memory_space=pltpu.HBM)] * 12,
        out_specs=vmem,
        scratch_shapes=[pltpu.VMEM((ROWS, TOK), BF16)] * 7
        + [pltpu.VMEM((8, 128), F32)] * 4
        + [
            pltpu.VMEM((4, ROWS, TOK), F32),
            pltpu.VMEM((HEADS, CH + EXTRA, 2 * CH), BF16),
            pltpu.VMEM((HEADS, 2 * CH, TOK), BF16),
            pltpu.VMEM((HEADS, CH, TOK), F32),
            pltpu.VMEM((SLABS, CH + EXTRA, 2 * CH), BF16),
            pltpu.VMEM((SLABS, TOK, TOK), F32),
            pltpu.VMEM((SLABS, CH // 2, 2 * CH), BF16),
            pltpu.VMEM((HEADS, CH // 2, 2 * CH), BF16),
            pltpu.VMEM((ROWS, TOK), BF16),
            pltpu.VMEM((4 * ROWS, ROWS), BF16),
            pltpu.VMEM((2 * pieces, CHUNK, TOK), F32),
            pltpu.VMEM((2 * pieces, CHUNK, TOK), F32),
            pltpu.VMEM((pieces, CHUNK, TOK), F32),
            pltpu.VMEM((pieces, CHUNK, TOK), BF16),
            pltpu.VMEM((pieces, CHUNK, TOK), BF16),
            pltpu.VMEM((ROWS, TOK), F32),
            pltpu.VMEM((HEADS, TOK, TOK), BF16),
            pltpu.VMEM((HEADS, TOK, TOK), BF16),
            pltpu.VMEM((BATCH, TOK, 2 * TOK), BF16),
            pltpu.VMEM((BATCH, TOK, TOK), BF16),
            pltpu.VMEM((BATCH, TOK, 2 * TOK), BF16),
            pltpu.VMEM((BATCH, TOK, 2 * TOK), BF16),
            pltpu.VMEM((BATCH, TOK, TOK), F32),
            pltpu.VMEM((BATCH, TOK, 2 * TOK), BF16),
            pltpu.VMEM((BATCH, TOK, TOK), F32),
            pltpu.VMEM((BATCH, CH, TOK), F32),
            pltpu.VMEM((BATCH, CH, TOK), F32),
            pltpu.VMEM((HEADS, TOK, 2 * TOK), BF16),
            pltpu.VMEM((HEADS, CH, TOK), F32),
            pltpu.VMEM((BATCH, 2 * TOK, 2 * TOK), BF16),
            dma((11,)),
            dma(()),
            dma((HEADS,)),
            dma((SLABS,)),
            dma((SLABS,)),
            dma((HEADS,)),
            dma((3 * pieces,)),
            dma((3 * pieces,)),
        ],
        compiler_params=pltpu.CompilerParams(
            collective_id=0, has_side_effects=True, vmem_limit_bytes=40 * 1024 * 1024
        ),
    )(*(
        pltpu.with_memory_space_constraint(x, pltpu.HBM) for x in (skip, r, k, v, g, w, a, *(p.reshape(8, 128) for p in (ef, rc, gm, gb)), wt)
    ))


def solution(mesh):
    split = P("head", "seq")
    vec = P("head")
    return jax.shard_map(
        on_device,
        mesh=mesh,
        in_specs=(split,) * 7 + (vec,) * 4 + (P(None, "head"),),
        out_specs=split,
        check_vma=False,
    )
```

```python
import functools
import jax
import jax.numpy as jnp
from jax import lax
from jax.experimental import pallas as pl
from jax.experimental.pallas import tpu as pltpu
from jax.sharding import PartitionSpec as P

MESH = pl.DeviceIdType.MESH
CH = 64
HEADS = 16
TOK = 128
SLABS = 32
ROWS = 1024
EXTRA = 16
GROUP = 8
LAG = 3
BATCH = 8
CHUNK = 128
F32 = jnp.float32
BF16 = jnp.bfloat16


def halves(x):
    high = x.astype(BF16)
    return high, (x - high.astype(F32)).astype(BF16)


def fold(x):
    return x[:, :TOK] + x[:, TOK:]


def mm(left, right):
    return jnp.dot(left, right, preferred_element_type=F32)


def kernel(
    skip_hbm, r_hbm, k_hbm, v_hbm, g_hbm, w_hbm, a_hbm, ef_hbm, rc_hbm, gm_hbm, gb_hbm, wt_hbm,
    out_ref,
    skip_ref, r_ref, k_ref, v_ref, g_ref, w_ref, a_ref, ef_ref, rc_ref, gm_ref, gb_ref,
    par, comb, read, local, inbox, prefix, outbox, entering, mixed, weights,
    send_a, got_a, held_b, send_b, got_b, total,
    pull_t, key_t, to_end, sums, ahead_s, pair_s, inv_s, inv, part_s, seen_s,
    recv_s, decay_s, solved_s, rest, both,
    in_sem, wt_sem, comb_send, comb_recv, state_send, state_recv, rs_send, rs_recv,
):
    head = lax.axis_index("head")
    me = lax.axis_index("seq")
    core = lax.rem(head, 2)
    chip = head // 2

    def owner_of(h):
        odd, place = h // 8, h % 8
        y = place // 2
        x = 2 * (place % 2) + (y + odd) % 2
        return y * 8 + x * 2 + (odd + core) % 2

    first = ((ef_hbm, ef_ref), (w_hbm, w_ref), (k_hbm, k_ref), (a_hbm, a_ref), (r_hbm, r_ref), (v_hbm, v_ref))
    second = ((rc_hbm, rc_ref), (gm_hbm, gm_ref), (gb_hbm, gb_ref), (g_hbm, g_ref), (skip_hbm, skip_ref))
    first = [pltpu.make_async_copy(*pair, in_sem.at[n]) for n, pair in enumerate(first)]
    second = [pltpu.make_async_copy(*pair, in_sem.at[6 + n]) for n, pair in enumerate(second)]
    wt_copy = pltpu.make_async_copy(wt_hbm, weights, wt_sem)
    for copy in first:
        copy.start()

    barrier = pltpu.get_barrier_semaphore()

    def greet(d, carry):
        pl.semaphore_signal(
            barrier, inc=1, device_id=(head, lax.rem(me + d, SLABS)), device_id_type=MESH
        )
        return carry

    lax.fori_loop(1, SLABS, greet, 0)

    def greet_head(d, carry):
        pl.semaphore_signal(
            barrier, inc=1, device_id=(lax.rem(head + d, 4), me), device_id_type=MESH
        )
        return carry

    lax.fori_loop(1, 4, greet_head, 0)

    def spread(p, ref):
        for j in range(8):
            par[p, j * 128 : (j + 1) * 128, :] = jnp.broadcast_to(ref[j : j + 1, :], (128, 128)).T

    for copy in first:
        copy.wait()
    for copy in second + [wt_copy]:
        copy.start()
    spread(0, ef_ref)

    row = lax.broadcasted_iota(jnp.int32, (TOK, TOK), 0)
    col = lax.broadcasted_iota(jnp.int32, (TOK, TOK), 1)
    upto = jnp.where(row <= col, 1.0, 0.0).astype(BF16)
    sums[...] = mm(w_ref[...], upto)
    apart = row ^ col
    near = (apart >= 2) & (apart < 16)
    zero = jnp.zeros((TOK, TOK), BF16)
    diag = lax.broadcasted_iota(jnp.int32, (CH, TOK), 0) == lax.broadcasted_iota(
        jnp.int32, (CH, TOK), 1
    )
    twice = row[:CH] == col[:CH] % CH
    left_half = lax.broadcasted_iota(jnp.int32, (CH, TOK), 1) < CH

    def wide(pair):
        return jnp.concatenate(
            [
                jnp.concatenate([pair[:, :TOK], pair[:, TOK:]], axis=1),
                jnp.concatenate([pair[:, :TOK], zero], axis=1),
            ],
            axis=0,
        )

    def beside(x):
        return jnp.concatenate(halves(x), axis=1)

    def turned(x):
        return jnp.concatenate(halves(x), axis=0).T

    def two_diag(one, other):
        return jnp.concatenate(
            [jnp.concatenate([one, zero], axis=1), jnp.concatenate([zero, other], axis=1)], axis=0
        )

    def stages(base):
        for i in range(BATCH):
            rows = slice((base + i) * CH, (base + i + 1) * CH)
            w16 = w_ref[rows, :]
            running = sums[rows, :]
            kf = k_ref[rows, :].astype(F32)
            scaled = kf * par[0, rows, :]
            removal = scaled * lax.rsqrt(jnp.sum(scaled * scaled, axis=0, keepdims=True) + 1e-6)
            pulled = removal * a_ref[rows, :].astype(F32)
            mid = running[:, 63:64]
            end = running[:, 127:128]
            back = jnp.exp(mid - running)
            at_mid = jnp.exp(mid)
            removal_fwd = -removal * jnp.exp(running - w16.astype(F32) - mid)
            pull_t[base + i] = turned(pulled * back)
            key_t[base + i] = turned(kf * back)
            to_end[base + i] = jnp.sum(jnp.where(twice, jnp.exp(end - mid), 0.0), axis=0, keepdims=True)
            rem_hi, rem_lo = halves(removal_fwd)
            ahead_s[base + i, :CH, :] = rem_hi
            ahead_s[base + i, CH:, :] = rem_lo
            seen_s[base + i, CH:, :] = removal_fwd * at_mid
            decay_s[base + i] = jnp.where(diag, jnp.exp(end), 0.0)
        yield
        for i in range(BATCH):
            ahead = ahead_s[base + i]
            ahead = jnp.concatenate([ahead[:CH], ahead[:CH], ahead[CH:], ahead[CH:]], axis=0)
            pull = pull_t[base + i]
            from_pull = mm(jnp.concatenate([pull, pull], axis=1), ahead)
            pair_mix = jnp.where(row < col, from_pull, 0.0)
            pair_s[base + i] = beside(jnp.where(apart >= 16, pair_mix, 0.0))
            inv[base + i] = jnp.where(apart < 16, pair_mix, 0.0)
            both[base + i, TOK:, :TOK] = jnp.where(apart == 1, pair_mix, 0.0).astype(BF16)
            both[base + i, :TOK, :TOK] = jnp.where(near, pair_mix, 0.0).astype(BF16)
            key = key_t[base + i]
            from_key = mm(jnp.concatenate([key, key], axis=1), ahead)
            part_s[base + i] = beside(jnp.where(row < col, from_key, 0.0))
        yield
        for i in range(BATCH):
            rows = slice((base + i) * CH, (base + i + 1) * CH)
            seen_s[base + i, :CH, :] = fold(mm(v_ref[rows, :], part_s[base + i]))
        yield
        for i in range(0, BATCH, 2):
            res = mm(
                jnp.concatenate([both[base + i, :TOK, :TOK], both[base + i + 1, :TOK, :TOK]], axis=1),
                two_diag(both[base + i, TOK:, :TOK], both[base + i + 1, TOK:, :TOK]),
            )
            for n in range(2):
                more = res[:, n * TOK : (n + 1) * TOK]
                both[base + i + n, :TOK, :TOK] = (both[base + i + n, :TOK, :TOK].astype(F32) + more).astype(BF16)
                inv[base + i + n] = inv[base + i + n] + more
        yield
        for turn in range(2):
            if turn:
                yield
            for i in range(0, BATCH, 2):
                res = mm(
                    jnp.concatenate([both[base + i, :, :TOK], both[base + i + 1, :, :TOK]], axis=1),
                    two_diag(both[base + i, :TOK, :TOK], both[base + i + 1, :TOK, :TOK]),
                )
                for n in range(2):
                    e = res[:TOK, n * TOK : (n + 1) * TOK]
                    m = inv[base + i + n] + res[TOK:, n * TOK : (n + 1) * TOK]
                    both[base + i + n, :TOK, :TOK] = e.astype(BF16)
                    both[base + i + n, TOK:, :TOK] = m.astype(BF16)
                    inv[base + i + n] = m + e
        yield
        for i in range(0, BATCH, 2):
            res = mm(
                jnp.concatenate([both[base + i, TOK:, :TOK], both[base + i + 1, TOK:, :TOK]], axis=1),
                two_diag(both[base + i, :TOK, :TOK], both[base + i + 1, :TOK, :TOK]),
            )
            for n in range(2):
                whole = jnp.where(row == col, 1.0, inv[base + i + n] + res[:, n * TOK : (n + 1) * TOK])
                inv_s[base + i + n] = beside(whole)
        yield
        for i in range(BATCH):
            left = jnp.concatenate([pair_s[base + i], beside(seen_s[base + i])], axis=0)
            res = fold(mm(left, wide(inv_s[base + i])))
            both[base + i] = beside(res)
            inv[base + i] = res[TOK:]
        yield
        for turn in range(2):
            if turn:
                yield
            for i in range(BATCH):
                res = fold(mm(both[base + i], wide(both[base + i, :TOK, :])))
                g = inv[base + i] + res[TOK:]
                both[base + i, :TOK, :] = beside(res[:TOK])
                both[base + i, TOK:, :] = beside(g)
                inv[base + i] = g
        yield
        for i in range(BATCH):
            solved_s[base + i] = beside(
                inv[base + i] + fold(mm(both[base + i, TOK:, :], wide(both[base + i, :TOK, :])))
            )
        yield
        for i in range(BATCH):
            h = base + i
            rows = slice(h * CH, (h + 1) * CH)
            pull = pull_t[h]
            ops = mm(solved_s[h], jnp.concatenate([pull, pull], axis=0))
            state = ops[:CH] + mm(v_ref[rows, :], key_t[h])
            trans = ops[CH:]
            state = (state + pltpu.roll(state, CH, 1)) * to_end[base + i]
            trans = (trans + pltpu.roll(trans, CH, 1)) * to_end[base + i] + decay_s[base + i]
            sent = jnp.where(left_half, trans, state).astype(BF16)
            comb[h, :CH, :] = sent
            missed = jnp.where(diag, trans - sent.astype(F32), 0.0)
            comb[h, CH:, :] = jnp.broadcast_to(
                jnp.sum(missed, axis=0, keepdims=True), (EXTRA, TOK)
            ).astype(BF16)

    def group_read(base):
        for i in range(BATCH):
            h = base + i
            rows = slice(h * CH, (h + 1) * CH)
            running = sums[rows, :]
            mid = running[:, 63:64]
            recept_fwd = r_ref[rows, :].astype(F32) * jnp.exp(running - mid)
            recv_s[i] = recept_fwd * jnp.exp(mid)
            high, low = halves(recept_fwd)
            ahead = jnp.concatenate([high, high, low, low], axis=0)
            pull, key = pull_t[h], key_t[h]
            pread = mm(jnp.concatenate([pull, pull], axis=1), ahead)
            kread = mm(jnp.concatenate([key, key], axis=1), ahead)
            pair_s[i] = beside(jnp.where(row <= col, pread, 0.0))
            part_s[i] = beside(jnp.where(row <= col, kread, 0.0))
        for i in range(BATCH):
            h = base + i
            rows = slice(h * CH, (h + 1) * CH)
            out = fold(mm(solved_s[h], wide(pair_s[i])))
            local[h] = out[:CH] + fold(mm(v_ref[rows, :], part_s[i]))
            read[h] = jnp.concatenate(halves(out[CH:] + recv_s[i]), axis=0)
            kf = k_ref[rows, :].astype(F32)
            vf = v_ref[rows, :].astype(F32)
            rf = r_ref[rows, :].astype(F32)
            bonus = jnp.sum(rf * kf * par[1, rows, :], axis=0, keepdims=True) * vf
            rest[h] = bonus + par[3, rows, :]

    def comb_copy(h):
        return pltpu.make_async_remote_copy(
            src_ref=comb.at[h],
            dst_ref=inbox.at[me],
            send_sem=comb_send.at[h],
            recv_sem=comb_recv.at[me],
            device_id=(head, owner_of(h)),
            device_id_type=MESH,
        )

    def send_comb(t, carry):
        h = (t // BATCH) * BATCH + (t + me + 3 * (me // 8)) % BATCH

        @pl.when(owner_of(h) != me)
        def _():
            comb_copy(h).start()

        @pl.when(owner_of(h) == me)
        def _():
            inbox[me] = comb[h]

        return carry

    ahead_of, behind = stages(0), stages(BATCH)
    for _ in range(LAG):
        next(ahead_of)
    running_on = True
    while running_on:
        running_on = next(ahead_of, True) is None
        if running_on:
            next(behind)
    pl.semaphore_wait(barrier, SLABS - 1 + 3)
    if LAG:
        lax.fori_loop(0, BATCH, send_comb, 0)
    for _ in behind:
        pass
    lax.fori_loop(BATCH if LAG else 0, HEADS, send_comb, 0)
    for copy in second:
        copy.wait()
    spread(1, rc_ref)
    spread(2, gm_ref)
    spread(3, gb_ref)
    for base in range(0, HEADS, BATCH):
        group_read(base)

    my_y, my_x = me // 8, (me // 2) % 4
    my_head = ((my_x + my_y) % 2) * 8 + 2 * my_y + my_x // 2

    def state_copy(i):
        return pltpu.make_async_remote_copy(
            src_ref=outbox.at[i],
            dst_ref=entering.at[my_head],
            send_sem=state_send.at[i],
            recv_sem=state_recv.at[my_head],
            device_id=(head, i),
            device_id_type=MESH,
        )

    @pl.when(owner_of(my_head) == me)
    def _():
        def arrive(d, carry):
            i = lax.rem(me + d, SLABS)
            pltpu.make_async_remote_copy(
                src_ref=comb.at[0],
                dst_ref=inbox.at[i],
                send_sem=comb_send.at[0],
                recv_sem=comb_recv.at[i],
                device_id=(head, i),
                device_id_type=MESH,
            ).wait_recv()
            return carry

        lax.fori_loop(1, SLABS, arrive, 0)

        def pack(i, value):
            half = CH // 2
            outbox[i] = jnp.where(left_half[:half], value[:half], value[half:]).astype(BF16)

        def item_of(i):
            item = inbox[i].astype(F32)
            swapped = pltpu.roll(item, CH, 1)
            trans = jnp.where(left_half, item[:CH], swapped[:CH])
            state = jnp.where(left_half, swapped[:CH], item[:CH])
            missed = jnp.where(left_half[:1], item[CH : CH + 1], swapped[CH : CH + 1])
            return trans, missed, state

        def left_of(x):
            return jnp.where(wide_half[: x.shape[0]], x, x - x.astype(BF16).astype(F32)).astype(BF16)

        def right_of(x):
            high, low = halves(x)
            none = jnp.zeros((CH, TOK), BF16)
            return jnp.concatenate(
                [jnp.concatenate([high, low], axis=1), jnp.concatenate([high, none], axis=1)],
                axis=0,
            )

        wide_half = lax.broadcasted_iota(jnp.int32, (TOK, TOK), 1) < CH
        groups = SLABS // GROUP
        for g in range(groups):
            trans, missed, state = item_of(g * GROUP)
            prefix[g * GROUP, :CH, :] = state
            prefix[g * GROUP, CH:, :] = trans + jnp.where((row % CH == col % CH)[:CH], missed, 0.0)

        def step(i, carry):
            for g in range(groups):
                trans, missed, state = item_of(g * GROUP + i)
                trans = trans.astype(BF16)
                old = prefix[g * GROUP + i - 1]
                moved = mm(left_of(old), jnp.concatenate([trans, trans], axis=0)) + old * missed
                prefix[g * GROUP + i, :CH, :] = moved[:CH] + state
                prefix[g * GROUP + i, CH:, :] = moved[CH:]
            return carry

        lax.fori_loop(1, GROUP, step, 0)
        start = jnp.zeros((CH, TOK), F32)
        starts = [start]
        for g in range(groups - 1):
            done = prefix[g * GROUP + GROUP - 1]
            start = done[:CH] if g == 0 else fold(mm(left_of(start), right_of(done[CH:]))) + done[:CH]
            starts.append(start)
        for g in range(groups):
            pack(g * GROUP, starts[g])
            for i in range(1, GROUP):
                done = prefix[g * GROUP + i - 1]
                moved = fold(mm(left_of(starts[g]), right_of(done[CH:]))) if g else 0.0
                pack(g * GROUP + i, moved + done[:CH])

        for _, dy, dx, dz in sorted(
            (-min(dy, 4 - dy) - min(dx, 4 - dx) - dz, dy, dx, dz)
            for dy in range(4)
            for dx in range(4)
            for dz in range(2)
            if dy + dx + dz
        ):
            state_copy((my_y + dy) % 4 * 8 + (my_x + dx) % 4 * 2 + (me + dz) % 2).start()
        entering[my_head] = outbox[me]

    def arrived(h):
        @pl.when(owner_of(h) != me)
        def _():
            pltpu.make_async_remote_copy(
                src_ref=outbox.at[0],
                dst_ref=entering.at[h],
                send_sem=state_send.at[0],
                recv_sem=state_recv.at[h],
                device_id=(head, owner_of(h)),
                device_id_type=MESH,
            ).wait_recv()

    for base in range(0, HEADS, BATCH):
        for i in range(BATCH):
            arrived(base + i)
        outs = []
        for i in range(BATCH):
            reading = read[base + i]
            state = entering[base + i]
            nil = jnp.zeros((CH, TOK), BF16)
            upper = jnp.concatenate([reading[:CH], nil, reading[CH:], nil], axis=0)
            lower = jnp.concatenate([nil, reading[:CH], nil, reading[CH:]], axis=0)
            y = mm(
                jnp.concatenate([state, state], axis=1),
                jnp.concatenate([upper, lower], axis=1),
            )
            outs.append(jnp.concatenate([y[:, :TOK], y[:, TOK:]], axis=0) + local[base + i])
        for i in range(BATCH):
            rows = slice((base + i) * CH, (base + i + 1) * CH)
            y = outs[i]
            centred = y - jnp.mean(y, axis=0, keepdims=True)
            spreading = jnp.mean(centred * centred, axis=0, keepdims=True)
            normed = centred * lax.rsqrt(spreading + 0.00064) * par[2, rows, :]
            mixed[rows, :] = ((normed + rest[base + i]) * g_ref[rows, :].astype(F32)).astype(BF16)

    wt_copy.wait()
    partner = chip * 2 + 1 - core
    across = (1 - chip) * 2 + core

    def piece(dest, c):
        rows = pl.ds(pl.multiple_of(dest * ROWS + c * CHUNK, CHUNK), CHUNK)
        return mm(weights[rows, :], mixed[...])

    pieces = ROWS // CHUNK

    def near_copy(c):
        return pltpu.make_async_remote_copy(
            src_ref=send_a.at[c],
            dst_ref=got_a.at[c],
            send_sem=rs_send.at[c],
            recv_sem=rs_recv.at[c],
            device_id=(partner, me),
            device_id_type=MESH,
        )

    def far_copy(c):
        return pltpu.make_async_remote_copy(
            src_ref=send_b.at[c],
            dst_ref=got_b.at[c],
            send_sem=rs_send.at[2 * pieces + c],
            recv_sem=rs_recv.at[2 * pieces + c],
            device_id=(across, me),
            device_id_type=MESH,
        )

    for c in range(pieces):
        send_a[c] = piece((1 - chip) * 2 + 1 - core, c)
        near_copy(c).start()
    for c in range(pieces):
        held_b[c] = piece(across, c)
        near_copy(c).wait_recv()
        send_b[c] = (held_b[c] + got_a[c]).astype(BF16)
        far_copy(c).start()
    for c in range(pieces):
        send_a[pieces + c] = piece(partner, c)
        near_copy(pieces + c).start()
    for c in range(pieces):
        rows = slice(c * CHUNK, (c + 1) * CHUNK)
        total[rows, :] = piece(head, c) + skip_ref[rows, :].astype(F32)
        near_copy(pieces + c).wait_recv()
        total[rows, :] = total[rows, :] + got_a[pieces + c]
    for c in range(2 * pieces):
        near_copy(c).wait_send()

    def sent_comb(h, carry):
        @pl.when(owner_of(h) != me)
        def _():
            comb_copy(h).wait_send()

        return carry

    lax.fori_loop(0, HEADS, sent_comb, 0)

    @pl.when(owner_of(my_head) == me)
    def _():
        def sent_state(d, carry):
            state_copy(lax.rem(me + d, SLABS)).wait_send()
            return carry

        lax.fori_loop(1, SLABS, sent_state, 0)

    for c in range(pieces):
        rows = slice(c * CHUNK, (c + 1) * CHUNK)
        far_copy(c).wait_recv()
        out_ref[rows, :] = (total[rows, :] + got_b[c].astype(F32)).astype(BF16)
    for c in range(pieces):
        far_copy(c).wait_send()


def on_device(skip, r, k, v, g, w, a, ef, rc, gm, gb, wt):
    vmem = pl.BlockSpec(memory_space=pltpu.VMEM)
    pieces = ROWS // CHUNK
    dma = pltpu.SemaphoreType.DMA
    return pl.pallas_call(
        kernel,
        out_shape=jax.ShapeDtypeStruct((ROWS, TOK), BF16),
        in_specs=[pl.BlockSpec(memory_space=pltpu.HBM)] * 12,
        out_specs=vmem,
        scratch_shapes=[pltpu.VMEM((ROWS, TOK), BF16)] * 7
        + [pltpu.VMEM((8, 128), F32)] * 4
        + [
            pltpu.VMEM((4, ROWS, TOK), F32),
            pltpu.VMEM((HEADS, CH + EXTRA, 2 * CH), BF16),
            pltpu.VMEM((HEADS, 2 * CH, TOK), BF16),
            pltpu.VMEM((HEADS, CH, TOK), F32),
            pltpu.VMEM((SLABS, CH + EXTRA, 2 * CH), BF16),
            pltpu.VMEM((SLABS, TOK, TOK), F32),
            pltpu.VMEM((SLABS, CH // 2, 2 * CH), BF16),
            pltpu.VMEM((HEADS, CH // 2, 2 * CH), BF16),
            pltpu.VMEM((ROWS, TOK), BF16),
            pltpu.VMEM((4 * ROWS, ROWS), BF16),
            pltpu.VMEM((2 * pieces, CHUNK, TOK), F32),
            pltpu.VMEM((2 * pieces, CHUNK, TOK), F32),
            pltpu.VMEM((pieces, CHUNK, TOK), F32),
            pltpu.VMEM((pieces, CHUNK, TOK), BF16),
            pltpu.VMEM((pieces, CHUNK, TOK), BF16),
            pltpu.VMEM((ROWS, TOK), F32),
            pltpu.VMEM((HEADS, TOK, TOK), BF16),
            pltpu.VMEM((HEADS, TOK, TOK), BF16),
            pltpu.VMEM((HEADS, 1, TOK), F32),
            pltpu.VMEM((ROWS, TOK), F32),
            pltpu.VMEM((HEADS, TOK, TOK), BF16),
            pltpu.VMEM((HEADS, TOK, 2 * TOK), BF16),
            pltpu.VMEM((HEADS, TOK, 2 * TOK), BF16),
            pltpu.VMEM((HEADS, TOK, TOK), F32),
            pltpu.VMEM((HEADS, TOK, 2 * TOK), BF16),
            pltpu.VMEM((HEADS, TOK, TOK), F32),
            pltpu.VMEM((HEADS, CH, TOK), F32),
            pltpu.VMEM((HEADS, CH, TOK), F32),
            pltpu.VMEM((HEADS, TOK, 2 * TOK), BF16),
            pltpu.VMEM((HEADS, CH, TOK), F32),
            pltpu.VMEM((HEADS, 2 * TOK, 2 * TOK), BF16),
            dma((11,)),
            dma(()),
            dma((HEADS,)),
            dma((SLABS,)),
            dma((SLABS,)),
            dma((HEADS,)),
            dma((3 * pieces,)),
            dma((3 * pieces,)),
        ],
        compiler_params=pltpu.CompilerParams(
            collective_id=0, has_side_effects=True, vmem_limit_bytes=40 * 1024 * 1024
        ),
    )(*(
        pltpu.with_memory_space_constraint(x, pltpu.HBM) for x in (skip, r, k, v, g, w, a, *(p.reshape(8, 128) for p in (ef, rc, gm, gb)), wt)
    ))


def solution(mesh):
    split = P("head", "seq")
    vec = P("head")
    return jax.shard_map(
        on_device,
        mesh=mesh,
        in_specs=(split,) * 7 + (vec,) * 4 + (P(None, "head"),),
        out_specs=split,
        check_vma=False,
    )
```

```python
import functools
import jax
import jax.numpy as jnp
from jax import lax
from jax.experimental import pallas as pl
from jax.experimental.pallas import tpu as pltpu
from jax.sharding import PartitionSpec as P

MESH = pl.DeviceIdType.MESH
CH = 64
HEADS = 16
TOK = 128
SLABS = 32
ROWS = 1024
EXTRA = 16
GROUP = 8
LAG = 3
BATCH = 8
CHUNK = 128
F32 = jnp.float32
BF16 = jnp.bfloat16


def halves(x):
    high = x.astype(BF16)
    return high, (x - high.astype(F32)).astype(BF16)


def fold(x):
    return x[:, :TOK] + x[:, TOK:]


def mm(left, right):
    return jnp.dot(left, right, preferred_element_type=F32)


def kernel(
    skip_hbm, r_hbm, k_hbm, v_hbm, g_hbm, w_hbm, a_hbm, ef_hbm, rc_hbm, gm_hbm, gb_hbm, wt_hbm,
    out_ref,
    skip_ref, r_ref, k_ref, v_ref, g_ref, w_ref, a_ref, ef_ref, rc_ref, gm_ref, gb_ref,
    par, comb, read, local, inbox, prefix, outbox, entering, mixed, weights,
    send_a, got_a, held_b, send_b, got_b, total,
    pull_t, key_t, to_end, sums, ahead_s, pair_s, inv_s, inv, part_s, seen_s,
    recv_s, decay_s, solved_s, rest, both,
    in_sem, wt_sem, comb_send, comb_recv, state_send, state_recv, rs_send, rs_recv,
):
    head = lax.axis_index("head")
    me = lax.axis_index("seq")
    core = lax.rem(head, 2)
    chip = head // 2

    def owner_of(h):
        odd, place = h // 8, h % 8
        y = place // 2
        x = 2 * (place % 2) + (y + odd) % 2
        return y * 8 + x * 2 + (odd + core) % 2

    first = ((ef_hbm, ef_ref), (w_hbm, w_ref), (k_hbm, k_ref), (a_hbm, a_ref), (r_hbm, r_ref), (v_hbm, v_ref))
    second = ((rc_hbm, rc_ref), (gm_hbm, gm_ref), (gb_hbm, gb_ref), (g_hbm, g_ref), (skip_hbm, skip_ref))
    first = [pltpu.make_async_copy(*pair, in_sem.at[n]) for n, pair in enumerate(first)]
    second = [pltpu.make_async_copy(*pair, in_sem.at[6 + n]) for n, pair in enumerate(second)]
    wt_copy = pltpu.make_async_copy(wt_hbm, weights, wt_sem)

    for copy in first:
        copy.start()

    barrier = pltpu.get_barrier_semaphore()

    for _, dy, dx, dz in sorted(
        (-min(dy, 4 - dy) - min(dx, 4 - dx) - dz, dy, dx, dz)
        for dy in range(4)
        for dx in range(4)
        for dz in range(2)
        if dy + dx + dz
    ):
        seat = (me // 8 + dy) % 4 * 8 + (me // 2 + dx) % 4 * 2 + (me + dz) % 2
        pl.semaphore_signal(barrier, inc=1, device_id=(head, seat), device_id_type=MESH)

    def greet_head(d, carry):
        pl.semaphore_signal(
            barrier, inc=1, device_id=(lax.rem(head + d, 4), me), device_id_type=MESH
        )
        return carry

    lax.fori_loop(1, 4, greet_head, 0)

    def spread(p, ref):
        for j in range(8):
            par[p, j * 128 : (j + 1) * 128, :] = jnp.broadcast_to(ref[j : j + 1, :], (128, 128)).T

    for copy in first:
        copy.wait()
    for copy in second + [wt_copy]:
        copy.start()
    spread(0, ef_ref)

    row = lax.broadcasted_iota(jnp.int32, (TOK, TOK), 0)
    col = lax.broadcasted_iota(jnp.int32, (TOK, TOK), 1)
    upto = jnp.where(row <= col, 1.0, 0.0).astype(BF16)
    sums[...] = mm(w_ref[...], upto)
    apart = row ^ col
    near = (apart >= 2) & (apart < 16)
    zero = jnp.zeros((TOK, TOK), BF16)
    diag = lax.broadcasted_iota(jnp.int32, (CH, TOK), 0) == lax.broadcasted_iota(
        jnp.int32, (CH, TOK), 1
    )
    twice = row[:CH] == col[:CH] % CH
    left_half = lax.broadcasted_iota(jnp.int32, (CH, TOK), 1) < CH

    def wide(pair):
        return jnp.concatenate(
            [
                jnp.concatenate([pair[:, :TOK], pair[:, TOK:]], axis=1),
                jnp.concatenate([pair[:, :TOK], zero], axis=1),
            ],
            axis=0,
        )

    def beside(x):
        return jnp.concatenate(halves(x), axis=1)

    def turned(x):
        return jnp.concatenate(halves(x), axis=0).T

    def two_diag(one, other):
        return jnp.concatenate(
            [jnp.concatenate([one, zero], axis=1), jnp.concatenate([zero, other], axis=1)], axis=0
        )

    def stages(base):
        for i in range(BATCH):
            rows = slice((base + i) * CH, (base + i + 1) * CH)
            w16 = w_ref[rows, :]
            running = sums[rows, :]
            kf = k_ref[rows, :].astype(F32)
            scaled = kf * par[0, rows, :]
            removal = scaled * lax.rsqrt(jnp.sum(scaled * scaled, axis=0, keepdims=True) + 1e-6)
            pulled = removal * a_ref[rows, :].astype(F32)
            mid = running[:, 63:64]
            end = running[:, 127:128]
            back = jnp.exp(mid - running)
            at_mid = jnp.exp(mid)
            removal_fwd = -removal * jnp.exp(running - w16.astype(F32) - mid)
            pull_t[base + i] = turned(pulled * back)
            key_t[base + i] = turned(kf * back)
            to_end[base + i] = jnp.sum(jnp.where(twice, jnp.exp(end - mid), 0.0), axis=0, keepdims=True)
            rem_hi, rem_lo = halves(removal_fwd)
            ahead_s[base + i, :CH, :] = rem_hi
            ahead_s[base + i, CH:, :] = rem_lo
            seen_s[base + i, CH:, :] = removal_fwd * at_mid
            decay_s[base + i] = jnp.where(diag, jnp.exp(end), 0.0)
        yield
        for i in range(BATCH):
            ahead = ahead_s[base + i]
            ahead = jnp.concatenate([ahead[:CH], ahead[:CH], ahead[CH:], ahead[CH:]], axis=0)
            pull = pull_t[base + i]
            from_pull = mm(jnp.concatenate([pull, pull], axis=1), ahead)
            pair_mix = jnp.where(row < col, from_pull, 0.0)
            pair_s[base + i] = beside(jnp.where(apart >= 16, pair_mix, 0.0))
            inv[base + i] = jnp.where(apart < 16, pair_mix, 0.0)
            both[base + i, TOK:, :TOK] = jnp.where(apart == 1, pair_mix, 0.0).astype(BF16)
            both[base + i, :TOK, :TOK] = jnp.where(near, pair_mix, 0.0).astype(BF16)
            key = key_t[base + i]
            from_key = mm(jnp.concatenate([key, key], axis=1), ahead)
            part_s[base + i] = beside(jnp.where(row < col, from_key, 0.0))
        yield
        for i in range(BATCH):
            rows = slice((base + i) * CH, (base + i + 1) * CH)
            seen_s[base + i, :CH, :] = fold(mm(v_ref[rows, :], part_s[base + i]))
        yield
        for i in range(0, BATCH, 2):
            res = mm(
                jnp.concatenate([both[base + i, :TOK, :TOK], both[base + i + 1, :TOK, :TOK]], axis=1),
                two_diag(both[base + i, TOK:, :TOK], both[base + i + 1, TOK:, :TOK]),
            )
            for n in range(2):
                more = res[:, n * TOK : (n + 1) * TOK]
                both[base + i + n, :TOK, :TOK] = (both[base + i + n, :TOK, :TOK].astype(F32) + more).astype(BF16)
                inv[base + i + n] = inv[base + i + n] + more
        yield
        for turn in range(2):
            if turn:
                yield
            for i in range(0, BATCH, 2):
                res = mm(
                    jnp.concatenate([both[base + i, :, :TOK], both[base + i + 1, :, :TOK]], axis=1),
                    two_diag(both[base + i, :TOK, :TOK], both[base + i + 1, :TOK, :TOK]),
                )
                for n in range(2):
                    e = res[:TOK, n * TOK : (n + 1) * TOK]
                    m = inv[base + i + n] + res[TOK:, n * TOK : (n + 1) * TOK]
                    both[base + i + n, :TOK, :TOK] = e.astype(BF16)
                    both[base + i + n, TOK:, :TOK] = m.astype(BF16)
                    inv[base + i + n] = m + e
        yield
        for i in range(0, BATCH, 2):
            res = mm(
                jnp.concatenate([both[base + i, TOK:, :TOK], both[base + i + 1, TOK:, :TOK]], axis=1),
                two_diag(both[base + i, :TOK, :TOK], both[base + i + 1, :TOK, :TOK]),
            )
            for n in range(2):
                whole = jnp.where(row == col, 1.0, inv[base + i + n] + res[:, n * TOK : (n + 1) * TOK])
                inv_s[base + i + n] = beside(whole)
        yield
        for i in range(BATCH):
            left = jnp.concatenate([pair_s[base + i], beside(seen_s[base + i])], axis=0)
            res = fold(mm(left, wide(inv_s[base + i])))
            both[base + i] = beside(res)
            inv[base + i] = res[TOK:]
        yield
        for turn in range(2):
            if turn:
                yield
            for i in range(BATCH):
                res = fold(mm(both[base + i], wide(both[base + i, :TOK, :])))
                g = inv[base + i] + res[TOK:]
                both[base + i, :TOK, :] = beside(res[:TOK])
                both[base + i, TOK:, :] = beside(g)
                inv[base + i] = g
        yield
        for i in range(BATCH):
            solved_s[base + i] = beside(
                inv[base + i] + fold(mm(both[base + i, TOK:, :], wide(both[base + i, :TOK, :])))
            )
        yield
        for i in range(BATCH):
            h = base + i
            rows = slice(h * CH, (h + 1) * CH)
            pull = pull_t[h]
            ops = mm(solved_s[h], jnp.concatenate([pull, pull], axis=0))
            state = ops[:CH] + mm(v_ref[rows, :], key_t[h])
            trans = ops[CH:]
            state = (state + pltpu.roll(state, CH, 1)) * to_end[base + i]
            trans = (trans + pltpu.roll(trans, CH, 1)) * to_end[base + i] + decay_s[base + i]
            sent = jnp.where(left_half, trans, state).astype(BF16)
            comb[h, :CH, :] = sent
            missed = jnp.where(diag, trans - sent.astype(F32), 0.0)
            comb[h, CH:, :] = jnp.broadcast_to(
                jnp.sum(missed, axis=0, keepdims=True), (EXTRA, TOK)
            ).astype(BF16)

    def group_read(base):
        for i in range(BATCH):
            h = base + i
            rows = slice(h * CH, (h + 1) * CH)
            running = sums[rows, :]
            mid = running[:, 63:64]
            recept_fwd = r_ref[rows, :].astype(F32) * jnp.exp(running - mid)
            recv_s[i] = recept_fwd * jnp.exp(mid)
            high, low = halves(recept_fwd)
            ahead = jnp.concatenate([high, high, low, low], axis=0)
            pull, key = pull_t[h], key_t[h]
            pread = mm(jnp.concatenate([pull, pull], axis=1), ahead)
            kread = mm(jnp.concatenate([key, key], axis=1), ahead)
            pair_s[i] = beside(jnp.where(row <= col, pread, 0.0))
            part_s[i] = beside(jnp.where(row <= col, kread, 0.0))
        for i in range(BATCH):
            h = base + i
            rows = slice(h * CH, (h + 1) * CH)
            out = fold(mm(solved_s[h], wide(pair_s[i])))
            local[h] = out[:CH] + fold(mm(v_ref[rows, :], part_s[i]))
            read[h] = jnp.concatenate(halves(out[CH:] + recv_s[i]), axis=0)
            kf = k_ref[rows, :].astype(F32)
            vf = v_ref[rows, :].astype(F32)
            rf = r_ref[rows, :].astype(F32)
            bonus = jnp.sum(rf * kf * par[1, rows, :], axis=0, keepdims=True) * vf
            rest[h] = bonus + par[3, rows, :]

    def comb_copy(h):
        return pltpu.make_async_remote_copy(
            src_ref=comb.at[h],
            dst_ref=inbox.at[me],
            send_sem=comb_send.at[h],
            recv_sem=comb_recv.at[me],
            device_id=(head, owner_of(h)),
            device_id_type=MESH,
        )

    def send_comb(t, carry):
        h = (t // BATCH) * BATCH + (t + me + 3 * (me // 8)) % BATCH

        @pl.when(owner_of(h) != me)
        def _():
            comb_copy(h).start()

        @pl.when(owner_of(h) == me)
        def _():
            inbox[me] = comb[h]

        return carry

    ahead_of, behind = stages(0), stages(BATCH)
    for _ in range(LAG):
        next(ahead_of)
    running_on = True
    while running_on:
        running_on = next(ahead_of, True) is None
        if running_on:
            next(behind)
    pl.semaphore_wait(barrier, SLABS - 1 + 3)
    if LAG:
        lax.fori_loop(0, BATCH, send_comb, 0)
    for _ in behind:
        pass
    lax.fori_loop(BATCH if LAG else 0, HEADS, send_comb, 0)
    for copy in second:
        copy.wait()
    spread(1, rc_ref)
    spread(2, gm_ref)
    spread(3, gb_ref)
    for base in range(0, HEADS, BATCH):
        group_read(base)

    my_y, my_x = me // 8, (me // 2) % 4
    my_head = ((my_x + my_y) % 2) * 8 + 2 * my_y + my_x // 2

    def state_copy(i):
        return pltpu.make_async_remote_copy(
            src_ref=outbox.at[i],
            dst_ref=entering.at[my_head],
            send_sem=state_send.at[i],
            recv_sem=state_recv.at[my_head],
            device_id=(head, i),
            device_id_type=MESH,
        )

    @pl.when(owner_of(my_head) == me)
    def _():
        def arrive(d, carry):
            i = lax.rem(me + d, SLABS)
            pltpu.make_async_remote_copy(
                src_ref=comb.at[0],
                dst_ref=inbox.at[i],
                send_sem=comb_send.at[0],
                recv_sem=comb_recv.at[i],
                device_id=(head, i),
                device_id_type=MESH,
            ).wait_recv()
            return carry

        lax.fori_loop(1, SLABS, arrive, 0)

        def pack(i, value):
            half = CH // 2
            outbox[i] = jnp.where(left_half[:half], value[:half], value[half:]).astype(BF16)

        def item_of(i):
            item = inbox[i].astype(F32)
            swapped = pltpu.roll(item, CH, 1)
            trans = jnp.where(left_half, item[:CH], swapped[:CH])
            state = jnp.where(left_half, swapped[:CH], item[:CH])
            missed = jnp.where(left_half[:1], item[CH : CH + 1], swapped[CH : CH + 1])
            return trans, missed, state

        def left_of(x):
            return jnp.where(wide_half[: x.shape[0]], x, x - x.astype(BF16).astype(F32)).astype(BF16)

        def right_of(x):
            high, low = halves(x)
            none = jnp.zeros((CH, TOK), BF16)
            return jnp.concatenate(
                [jnp.concatenate([high, low], axis=1), jnp.concatenate([high, none], axis=1)],
                axis=0,
            )

        wide_half = lax.broadcasted_iota(jnp.int32, (TOK, TOK), 1) < CH
        groups = SLABS // GROUP
        for g in range(groups):
            trans, missed, state = item_of(g * GROUP)
            prefix[g * GROUP, :CH, :] = state
            prefix[g * GROUP, CH:, :] = trans + jnp.where((row % CH == col % CH)[:CH], missed, 0.0)

        def step(i, carry):
            for g in range(groups):
                trans, missed, state = item_of(g * GROUP + i)
                trans = trans.astype(BF16)
                old = prefix[g * GROUP + i - 1]
                moved = mm(left_of(old), jnp.concatenate([trans, trans], axis=0)) + old * missed
                prefix[g * GROUP + i, :CH, :] = moved[:CH] + state
                prefix[g * GROUP + i, CH:, :] = moved[CH:]
            return carry

        lax.fori_loop(1, GROUP, step, 0)
        start = jnp.zeros((CH, TOK), F32)
        starts = [start]
        for g in range(groups - 1):
            done = prefix[g * GROUP + GROUP - 1]
            start = done[:CH] if g == 0 else fold(mm(left_of(start), right_of(done[CH:]))) + done[:CH]
            starts.append(start)
        for g in range(groups):
            pack(g * GROUP, starts[g])
            for i in range(1, GROUP):
                done = prefix[g * GROUP + i - 1]
                moved = fold(mm(left_of(starts[g]), right_of(done[CH:]))) if g else 0.0
                pack(g * GROUP + i, moved + done[:CH])

        for _, dy, dx, dz in sorted(
            (-min(dy, 4 - dy) - min(dx, 4 - dx) - dz, dy, dx, dz)
            for dy in range(4)
            for dx in range(4)
            for dz in range(2)
            if dy + dx + dz
        ):
            state_copy((my_y + dy) % 4 * 8 + (my_x + dx) % 4 * 2 + (me + dz) % 2).start()
        entering[my_head] = outbox[me]

    def arrived(h):
        @pl.when(owner_of(h) != me)
        def _():
            pltpu.make_async_remote_copy(
                src_ref=outbox.at[0],
                dst_ref=entering.at[h],
                send_sem=state_send.at[0],
                recv_sem=state_recv.at[h],
                device_id=(head, owner_of(h)),
                device_id_type=MESH,
            ).wait_recv()

    for base in range(0, HEADS, BATCH):
        for i in range(BATCH):
            arrived(base + i)
        outs = []
        for i in range(BATCH):
            reading = read[base + i]
            state = entering[base + i]
            nil = jnp.zeros((CH, TOK), BF16)
            upper = jnp.concatenate([reading[:CH], nil, reading[CH:], nil], axis=0)
            lower = jnp.concatenate([nil, reading[:CH], nil, reading[CH:]], axis=0)
            y = mm(
                jnp.concatenate([state, state], axis=1),
                jnp.concatenate([upper, lower], axis=1),
            )
            outs.append(jnp.concatenate([y[:, :TOK], y[:, TOK:]], axis=0) + local[base + i])
        for i in range(BATCH):
            rows = slice((base + i) * CH, (base + i + 1) * CH)
            y = outs[i]
            centred = y - jnp.mean(y, axis=0, keepdims=True)
            spreading = jnp.mean(centred * centred, axis=0, keepdims=True)
            normed = centred * lax.rsqrt(spreading + 0.00064) * par[2, rows, :]
            mixed[rows, :] = ((normed + rest[base + i]) * g_ref[rows, :].astype(F32)).astype(BF16)

    wt_copy.wait()
    partner = chip * 2 + 1 - core
    across = (1 - chip) * 2 + core

    def piece(dest, c):
        rows = pl.ds(pl.multiple_of(dest * ROWS + c * CHUNK, CHUNK), CHUNK)
        return mm(weights[rows, :], mixed[...])

    pieces = ROWS // CHUNK

    def near_copy(c):
        return pltpu.make_async_remote_copy(
            src_ref=send_a.at[c],
            dst_ref=got_a.at[c],
            send_sem=rs_send.at[c],
            recv_sem=rs_recv.at[c],
            device_id=(partner, me),
            device_id_type=MESH,
        )

    def far_copy(c):
        return pltpu.make_async_remote_copy(
            src_ref=send_b.at[c],
            dst_ref=got_b.at[c],
            send_sem=rs_send.at[2 * pieces + c],
            recv_sem=rs_recv.at[2 * pieces + c],
            device_id=(across, me),
            device_id_type=MESH,
        )

    for c in range(pieces):
        send_a[c] = piece((1 - chip) * 2 + 1 - core, c)
        near_copy(c).start()
    for c in range(pieces):
        held_b[c] = piece(across, c)
        near_copy(c).wait_recv()
        send_b[c] = (held_b[c] + got_a[c]).astype(BF16)
        far_copy(c).start()
    for c in range(pieces):
        send_a[pieces + c] = piece(partner, c)
        near_copy(pieces + c).start()
    for c in range(pieces):
        rows = slice(c * CHUNK, (c + 1) * CHUNK)
        total[rows, :] = piece(head, c) + skip_ref[rows, :].astype(F32)
        near_copy(pieces + c).wait_recv()
        total[rows, :] = total[rows, :] + got_a[pieces + c]
    for c in range(2 * pieces):
        near_copy(c).wait_send()

    def sent_comb(h, carry):
        @pl.when(owner_of(h) != me)
        def _():
            comb_copy(h).wait_send()

        return carry

    lax.fori_loop(0, HEADS, sent_comb, 0)

    @pl.when(owner_of(my_head) == me)
    def _():
        def sent_state(d, carry):
            state_copy(lax.rem(me + d, SLABS)).wait_send()
            return carry

        lax.fori_loop(1, SLABS, sent_state, 0)

    for c in range(pieces):
        rows = slice(c * CHUNK, (c + 1) * CHUNK)
        far_copy(c).wait_recv()
        out_ref[rows, :] = (total[rows, :] + got_b[c].astype(F32)).astype(BF16)
    for c in range(pieces):
        far_copy(c).wait_send()


def on_device(skip, r, k, v, g, w, a, ef, rc, gm, gb, wt):
    vmem = pl.BlockSpec(memory_space=pltpu.VMEM)
    pieces = ROWS // CHUNK
    dma = pltpu.SemaphoreType.DMA
    return pl.pallas_call(
        kernel,
        out_shape=jax.ShapeDtypeStruct((ROWS, TOK), BF16),
        in_specs=[pl.BlockSpec(memory_space=pltpu.HBM)] * 12,
        out_specs=vmem,
        scratch_shapes=[pltpu.VMEM((ROWS, TOK), BF16)] * 7
        + [pltpu.VMEM((8, 128), F32)] * 4
        + [
            pltpu.VMEM((4, ROWS, TOK), F32),
            pltpu.VMEM((HEADS, CH + EXTRA, 2 * CH), BF16),
            pltpu.VMEM((HEADS, 2 * CH, TOK), BF16),
            pltpu.VMEM((HEADS, CH, TOK), F32),
            pltpu.VMEM((SLABS, CH + EXTRA, 2 * CH), BF16),
            pltpu.VMEM((SLABS, TOK, TOK), F32),
            pltpu.VMEM((SLABS, CH // 2, 2 * CH), BF16),
            pltpu.VMEM((HEADS, CH // 2, 2 * CH), BF16),
            pltpu.VMEM((ROWS, TOK), BF16),
            pltpu.VMEM((4 * ROWS, ROWS), BF16),
            pltpu.VMEM((2 * pieces, CHUNK, TOK), F32),
            pltpu.VMEM((2 * pieces, CHUNK, TOK), F32),
            pltpu.VMEM((pieces, CHUNK, TOK), F32),
            pltpu.VMEM((pieces, CHUNK, TOK), BF16),
            pltpu.VMEM((pieces, CHUNK, TOK), BF16),
            pltpu.VMEM((ROWS, TOK), F32),
            pltpu.VMEM((HEADS, TOK, TOK), BF16),
            pltpu.VMEM((HEADS, TOK, TOK), BF16),
            pltpu.VMEM((HEADS, 1, TOK), F32),
            pltpu.VMEM((ROWS, TOK), F32),
            pltpu.VMEM((HEADS, TOK, TOK), BF16),
            pltpu.VMEM((HEADS, TOK, 2 * TOK), BF16),
            pltpu.VMEM((HEADS, TOK, 2 * TOK), BF16),
            pltpu.VMEM((HEADS, TOK, TOK), F32),
            pltpu.VMEM((HEADS, TOK, 2 * TOK), BF16),
            pltpu.VMEM((HEADS, TOK, TOK), F32),
            pltpu.VMEM((HEADS, CH, TOK), F32),
            pltpu.VMEM((HEADS, CH, TOK), F32),
            pltpu.VMEM((HEADS, TOK, 2 * TOK), BF16),
            pltpu.VMEM((HEADS, CH, TOK), F32),
            pltpu.VMEM((HEADS, 2 * TOK, 2 * TOK), BF16),
            dma((11,)),
            dma(()),
            dma((HEADS,)),
            dma((SLABS,)),
            dma((SLABS,)),
            dma((HEADS,)),
            dma((3 * pieces,)),
            dma((3 * pieces,)),
        ],
        compiler_params=pltpu.CompilerParams(
            collective_id=0, has_side_effects=True, vmem_limit_bytes=40 * 1024 * 1024
        ),
    )(*(
        pltpu.with_memory_space_constraint(x, pltpu.HBM) for x in (skip, r, k, v, g, w, a, *(p.reshape(8, 128) for p in (ef, rc, gm, gb)), wt)
    ))


def solution(mesh):
    split = P("head", "seq")
    vec = P("head")
    return jax.shard_map(
        on_device,
        mesh=mesh,
        in_specs=(split,) * 7 + (vec,) * 4 + (P(None, "head"),),
        out_specs=split,
        check_vma=False,
    )
```
